32 devices in a mesh: rep: 2 (over x), ctx: 16 (over z, y, core).
Axes of the slice: x: 2, y: 2, z: 4, core: 2. Of those that a mesh axis runs over, the one named last changes fastest.
Arguments:
- queries: bfloat16 [4096, 32, 128], P(('rep', 'ctx')), parts along dimension 0, may hold values from -128 to 128
- keys: bfloat16 [4096, 2, 128], P(('rep', 'ctx')), parts along dimension 0, may hold values from -5 to 5
- values: bfloat16 [4096, 2, 128], P(('rep', 'ctx')), parts along dimension 0, may hold values from -6 to 6
- grad_out: bfloat16 [4096, 32, 128], P(('rep', 'ctx')), parts along dimension 0, may hold values from -6 to 6
- selected: int32 [4096, 2, 8], P(('rep', 'ctx')), parts along dimension 0, may hold values from 0 to 31, as said below
Outputs:
- dquery: bfloat16 [4096, 32, 128], P(('rep', 'ctx')), parts along dimension 0
- key_grad: bfloat16 [4096, 2, 128], P(('rep', 'ctx')), parts along dimension 0
- value_grad: bfloat16 [4096, 2, 128], P(('rep', 'ctx')), parts along dimension 0
The draws below stay inside these ranges and needn't reach their ends.
There are 2 independent parts, one for each index of `rep`. The reference program is written for one: setup_inputs(seed, part) draws one part's arguments, and reference() takes and returns one part's arrays. A program takes and returns all parts, laid end to end along the dimension named above; each array names one. Nothing has to cross between parts.
Inputs may be any that keep to these rules, and one draw needn't show every extreme that they name: The 8 blocks of selected[t, g] are different and include block t // 64 and block 0. Over the 128 tokens of one device of ctx, the blocks named for one group that lie on other devices number exactly 7, at most one of each other device; block 0 is among them for every device but the first.
All inputs are finite; a program needn't handle non-finite values.
Results may differ from the reference program's by a relative error of at most 0.0075.
Values may be sent and summed in bfloat16 or wider, within the bound.
A program may use at most 128 MiB of HBM per device.

```python
import math
import jax
import jax.numpy as jnp
from jax import lax

HEADS = 32
KVG = 2
DH = 128
BLK = 64
SEL = 8
TOK_DEV = 128
BPD = 2
OTHERS = 6
FG = 7
POOLB = 9
SEQ = 2048
N_CTX = 16


def choose_blocks(key):
    base = jax.random.fold_in(key, 11)
    first, second, third, fourth = jax.random.split(base, 4)
    requesters = jnp.arange(N_CTX).astype(jnp.int32)[:, None]
    owner_ids = jnp.arange(N_CTX).astype(jnp.int32)[None, :]
    noise = jax.random.randint(first, (N_CTX, N_CTX), 0, 1 << 20)
    ranking = noise * N_CTX + owner_ids + jnp.where(owner_ids < requesters, 1 << 27, 0)
    ranking = jnp.where((owner_ids == requesters) | (owner_ids == 0), -1, ranking)
    unused, ranked = lax.top_k(ranking, FG)
    with_sink = jnp.concatenate([jnp.zeros((N_CTX, 1), jnp.int32), ranked[:, :OTHERS]], axis=1)
    owner_list = jnp.where(requesters > 0, with_sink, ranked).astype(jnp.int32)
    local_ids = jax.random.randint(second, (N_CTX, FG, KVG), 0, BPD)
    local_ids = jnp.where(owner_list[..., None] == 0, 0, local_ids)
    far_blocks = owner_list[..., None] * BPD + local_ids
    own_blocks = requesters * BPD + jnp.arange(BPD).astype(jnp.int32)[None, :]
    own_blocks = jnp.broadcast_to(own_blocks[:, :, None], (N_CTX, BPD, KVG))
    pool_ids = jnp.concatenate([own_blocks, far_blocks], axis=1).transpose(0, 2, 1)
    pool_tokens = jnp.repeat(pool_ids, TOK_DEV, axis=0)
    token_ids = jnp.arange(SEQ).astype(jnp.int32)
    slot_ids = jnp.arange(POOLB).astype(jnp.int32)
    needed = (pool_tokens == (token_ids // BLK)[:, None, None]) | (pool_tokens == 0)
    needed = needed | (slot_ids[None, None, :] == (token_ids % TOK_DEV % POOLB)[:, None, None])
    shuffle = jax.random.randint(third, (SEQ, KVG, POOLB), 0, 1 << 20)
    marks = shuffle * POOLB + slot_ids + jnp.where(needed, 1 << 26, 0)
    unused_top, picks = lax.top_k(marks, SEL)
    chosen = jnp.take_along_axis(pool_tokens, picks, axis=2)
    reorder = jax.random.randint(fourth, (SEQ, KVG, SEL), 0, 1 << 20) * SEL + jnp.arange(SEL).astype(jnp.int32)
    order = jnp.argsort(reorder, axis=2)
    return jnp.take_along_axis(chosen, order, axis=2).astype(jnp.int32)


def query_key_pair(key):
    base = jax.random.fold_in(key, 23)
    first, second = jax.random.split(base, 2)
    key_base = jnp.clip(jax.random.normal(first, (SEQ, KVG, DH), jnp.float32), -5.0, 5.0)
    key_vals = key_base
    query_vals = jnp.clip(2.0 * jax.random.normal(second, (SEQ, HEADS, DH), jnp.float32), -12.0, 12.0)
    return (query_vals, key_vals)


def draw_queries(key, part):
    query_vals, key_vals = query_key_pair(key)
    return query_vals.astype(jnp.bfloat16)


def draw_keys(key, part):
    query_vals, key_vals = query_key_pair(key)
    return key_vals.astype(jnp.bfloat16)


def draw_selected(key, part):
    return choose_blocks(key)


def block_levels(stream_key, shape, cuts, low, largest):
    level, own = 1.0, jax.random.fold_in(stream_key, 6)
    for position, blocks in cuts:
        draws = jnp.exp(jax.random.uniform(jax.random.fold_in(own, position), (blocks,), jnp.float32, low / len(cuts), largest / len(cuts)))
        level = level * jnp.repeat(draws, shape[position] // blocks).reshape([-1 if axis == position else 1 for axis in range(len(shape))])
    return level


def normal_values(stream_key, dims, deviation, reach, cuts=(), held_as=jnp.bfloat16):
    entries = jax.random.normal(stream_key, dims, jnp.float32) * deviation
    if len(cuts) > 0:
        entries = block_levels(stream_key, dims, cuts, -0.22, 0.18) * entries
    return jnp.clip(entries, min=-reach, max=reach).astype(held_as)


def setup_inputs(seed: int = 0, part: int = 0) -> dict:
    splits = jax.random.split(jax.random.key(seed), 6)
    own_keys = jax.random.split(jax.random.fold_in(splits[5], part), 6)
    return {
        "queries": draw_queries(jax.random.fold_in(jax.random.fold_in(splits[5], part), 71), part),
        "keys": draw_keys(jax.random.fold_in(jax.random.fold_in(splits[5], part), 71), part),
        "values": normal_values(own_keys[2], (SEQ, KVG, DH), 1.0, 6.0, ((0, 16),)),
        "grad_out": normal_values(own_keys[3], (SEQ, HEADS, DH), 1.0, 6.0, ((0, 16),)),
        "selected": draw_selected(jax.random.fold_in(jax.random.fold_in(splits[5], part), 71), part),
    }


def reference(queries, keys, values, grad_out, selected):
    seq_len, head_count, head_dim = queries.shape
    groups = keys.shape[1]
    per_group = head_count // groups
    scaling = 1.0 / math.sqrt(head_dim)
    tile_rows = min(seq_len, 64)
    step_count = seq_len // tile_rows
    keys_by_group = keys.transpose(1, 0, 2)
    values_by_group = values.transpose(1, 0, 2)
    group_ids = jnp.arange(groups).astype(jnp.int32)[None, :, None]
    offsets = jnp.arange(BLK).astype(jnp.int32)

    def visit(carry, inputs):
        key_acc, value_acc = carry
        query_blk, upstream, chosen, first = inputs
        positions = (chosen[..., None] * BLK + offsets).reshape(tile_rows, groups, -1).astype(jnp.int32)
        key_rows = keys_by_group[group_ids, positions].astype(jnp.float32)
        value_rows = values_by_group[group_ids, positions].astype(jnp.float32)
        query_f = query_blk.astype(jnp.float32).reshape(tile_rows, groups, per_group, head_dim)
        upstream_f = upstream.astype(jnp.float32).reshape(tile_rows, groups, per_group, head_dim)
        scores = jnp.einsum('tghd,tgld->tghl', query_f, key_rows) * scaling
        query_pos = first + jnp.arange(tile_rows).astype(jnp.int32)
        allowed = positions <= query_pos[:, None, None]
        scores = jnp.where(allowed[:, :, None, :], scores, -jnp.inf)
        row_peak = lax.optimization_barrier(jnp.max(scores, axis=-1, keepdims=True))
        weights = jnp.exp(scores - row_peak)
        weights = weights / lax.optimization_barrier(jnp.sum(weights, axis=-1, keepdims=True))
        slope_grad = jnp.einsum('tghd,tgld->tghl', upstream_f, value_rows)
        row_inner = lax.optimization_barrier(jnp.sum(weights * slope_grad, axis=-1, keepdims=True))
        dscore = lax.optimization_barrier((weights * (slope_grad - row_inner) * scaling).astype(jnp.bfloat16))
        weights_low = lax.optimization_barrier(weights.astype(jnp.bfloat16))
        dscore_f = dscore.astype(jnp.float32)
        weights_f = weights_low.astype(jnp.float32)
        dquery = jnp.einsum('tghl,tgld->tghd', dscore_f, key_rows).astype(jnp.bfloat16)
        key_part = jnp.einsum('tghl,tghd->tgld', dscore_f, query_f)
        value_part = jnp.einsum('tghl,tghd->tgld', weights_f, upstream_f)
        key_acc = key_acc.at[group_ids, positions].add(key_part)
        value_acc = value_acc.at[group_ids, positions].add(value_part)
        return ((key_acc, value_acc), dquery.reshape(tile_rows, head_count, head_dim))
    inputs = (queries.reshape(step_count, tile_rows, head_count, head_dim), grad_out.reshape(step_count, tile_rows, head_count, head_dim), selected.reshape(step_count, tile_rows, groups, -1), (jnp.arange(step_count) * tile_rows).astype(jnp.int32))
    zeros_init = jnp.zeros((groups, seq_len, head_dim), jnp.float32)
    (key_acc, value_acc), dquery = lax.scan(visit, (zeros_init, zeros_init), inputs)
    dquery = dquery.reshape(seq_len, head_count, head_dim)
    key_grad = key_acc.transpose(1, 0, 2).astype(jnp.bfloat16)
    value_grad = value_acc.transpose(1, 0, 2).astype(jnp.bfloat16)
    return (dquery, key_grad, value_grad)
```

```python
import functools
import math

import jax
import jax.numpy as jnp
from jax import lax
from jax.experimental import pallas as pl
from jax.experimental.pallas import tpu as pltpu
from jax.sharding import PartitionSpec as P

BLK = 64
NEG = -1e30
ID_ROWS = 16
LOG2E = math.log2(math.e)
NT = (((1,), (1,)), ((), ()))
NN = (((1,), (0,)), ((), ()))


def barrier_all(n, me):
    barrier = pltpu.get_barrier_semaphore()

    def greet(k, carry):
        peer = lax.rem(me + k, n)
        pl.semaphore_signal(
            barrier, inc=1, device_id={"ctx": peer}, device_id_type=pl.DeviceIdType.MESH
        )
        return carry

    lax.fori_loop(1, n, greet, 0)
    pl.semaphore_wait(barrier, n - 1)


def gather_kernel(n, kv_ref, out_ref, send_sem, fwd_sem, recv_sem, local_sem):
    me = lax.axis_index("ctx")
    sib = me + 1 - 2 * lax.rem(me, 2)
    half = n // 2
    barrier_all(n, me)

    def direct(k):
        return pltpu.make_async_remote_copy(
            src_ref=kv_ref,
            dst_ref=out_ref.at[me],
            send_sem=send_sem.at[k],
            recv_sem=recv_sem.at[me],
            device_id={"ctx": lax.rem(me + 2 * k, n)},
            device_id_type=pl.DeviceIdType.MESH,
        )

    def forward(src):
        return pltpu.make_async_remote_copy(
            src_ref=out_ref.at[src],
            dst_ref=out_ref.at[src],
            send_sem=fwd_sem.at[src],
            recv_sem=recv_sem.at[src],
            device_id={"ctx": sib},
            device_id_type=pl.DeviceIdType.MESH,
        )

    def arrival(src):
        return pltpu.make_async_remote_copy(
            src_ref=kv_ref,
            dst_ref=out_ref.at[src],
            send_sem=send_sem.at[0],
            recv_sem=recv_sem.at[src],
            device_id={"ctx": sib},
            device_id_type=pl.DeviceIdType.MESH,
        )

    to_sib = pltpu.make_async_remote_copy(
        src_ref=kv_ref,
        dst_ref=out_ref.at[me],
        send_sem=send_sem.at[0],
        recv_sem=recv_sem.at[me],
        device_id={"ctx": sib},
        device_id_type=pl.DeviceIdType.MESH,
    )

    @pl.loop(1, half)
    def _(k):
        direct(k).start()

    to_sib.start()
    own = pltpu.make_async_copy(kv_ref, out_ref.at[me], local_sem)
    own.start()

    @pl.loop(1, half)
    def _(k):
        src = lax.rem(me + 2 * (half - k), n)
        arrival(src).wait_recv()
        forward(src).start()

    @pl.loop(0, half)
    def _(k):
        arrival(lax.rem(sib + 2 * k, n)).wait_recv()

    own.wait()
    to_sib.wait_send()

    @pl.loop(1, half)
    def _(k):
        direct(k).wait_send()
        forward(lax.rem(me + 2 * (half - k), n)).wait_send()


def attend(g, per_group, chunk_tokens, picked_ref, q_ref, do_ref, dq_ref, pool_ref, acc_ref):
    tokens, _, dh = q_ref.shape
    own_rows = tokens
    keys = pool_ref.shape[1]
    slots = keys // BLK
    own_slots = own_rows // BLK
    scaling = 1.0 / math.sqrt(dh)
    log_scale = scaling * LOG2E
    rows = chunk_tokens * per_group
    shift = per_group.bit_length() - 1
    pool_k = pool_ref[0]
    pool_v = pool_ref[1]
    pool_kt = pool_k.T
    acc_ref[...] = jnp.zeros_like(acc_ref)
    heads = slice(g * per_group, (g + 1) * per_group)

    @pl.loop(0, tokens // chunk_tokens)
    def _(c):
        t0 = pl.multiple_of(c * chunk_tokens, chunk_tokens)
        q = q_ref[pl.ds(t0, chunk_tokens), heads, :].reshape(rows, dh)
        do = do_ref[pl.ds(t0, chunk_tokens), heads, :].reshape(rows, dh)
        row_tok = t0 + (lax.broadcasted_iota(jnp.int32, (tokens, rows), 1) >> shift)
        tok = lax.broadcasted_iota(jnp.int32, (tokens, rows), 0)
        spread = jnp.where(row_tok == tok, 1.0, 0.0).astype(jnp.bfloat16)
        seen = lax.dot_general(picked_ref[g], spread, NN, preferred_element_type=jnp.float32)
        bias = (seen - 1.0) * (-NEG)
        s = lax.dot_general(pool_k, q, NT, preferred_element_type=jnp.float32)
        dp = lax.dot_general(pool_v, do, NT, preferred_element_type=jnp.float32)
        pieces = []
        for j in range(slots):
            piece = s[j * BLK : (j + 1) * BLK] + bias[j : j + 1]
            if j < own_slots:
                key_pos = j * BLK + lax.broadcasted_iota(jnp.int32, (BLK, rows), 0)
                causal = key_pos <= row_tok[:BLK]
                piece = jnp.where(causal, piece, NEG)
            pieces.append(piece)
        s = jnp.concatenate(pieces, axis=0)
        peak = jnp.max(s, axis=0, keepdims=True)
        e = jnp.exp2((s - peak) * log_scale)
        total = jnp.sum(e, axis=0, keepdims=True)
        weighted = jnp.sum(e * dp, axis=0, keepdims=True)
        inv = 1.0 / total
        inner = weighted * inv
        p = e * inv
        ds = (p * (dp - inner)).astype(jnp.bfloat16)
        p = p.astype(jnp.bfloat16)
        dqt = lax.dot_general(pool_kt, ds, NN, preferred_element_type=jnp.float32)
        dq = (dqt * scaling).T.astype(jnp.bfloat16)
        dq_ref[pl.ds(t0, chunk_tokens), heads, :] = dq.reshape(chunk_tokens, per_group, dh)
        acc_ref[0] += lax.dot_general(ds, q, NN, preferred_element_type=jnp.float32)
        acc_ref[1] += lax.dot_general(p, do, NN, preferred_element_type=jnp.float32)

    acc_ref[0] = acc_ref[0] * scaling


def fill_pool(g, n_far, far_owner, far_block, own_kv, gathered_ref, pool_ref):
    own_rows = own_kv.shape[2]
    pool_ref[:, :own_rows, :] = own_kv[g]
    for s in range(n_far):
        owner = far_owner[g, s]
        start = pl.multiple_of(far_block[g, s] * BLK, BLK)
        lo = own_rows + s * BLK
        for kv in range(2):
            pool_ref[kv, lo : lo + BLK, :] = gathered_ref[owner, g, kv, pl.ds(start, BLK), :]


def fill_outbox(g, n, own_rows, slot_of, live, block_of, acc_ref, outbox):
    def fill(j, carry):
        start = pl.multiple_of(own_rows + slot_of[g, j] * BLK, BLK)
        keep = live[g, j].astype(jnp.float32)
        base = ID_ROWS + g * 2 * BLK
        for kv in range(2):
            part = acc_ref[kv, pl.ds(start, BLK), :] * keep
            outbox[j, base + kv * BLK : base + (kv + 1) * BLK, :] = part.astype(jnp.bfloat16)
        return carry

    lax.fori_loop(0, n, fill, 0)


def fill_ids(n, groups, block_of, outbox):
    dh = outbox.shape[2]

    def fill(j, carry):
        row = lax.broadcasted_iota(jnp.int32, (ID_ROWS, dh), 0)
        ids = jnp.zeros((ID_ROWS, dh), jnp.float32)
        for g in range(groups):
            ids = jnp.where(row == g, block_of[g, j].astype(jnp.float32), ids)
        outbox[j, :ID_ROWS, :] = ids.astype(jnp.bfloat16)
        return carry

    lax.fori_loop(0, n, fill, 0)


def attend_kernel(
    n, n_far, chunk_tokens,
    far_owner, far_block, slot_of, live, block_of,
    picked_ref, q_ref, do_ref, own_kv, gathered_ref,
    dq_ref, outbox, own_grad, pool_ref, acc_ref,
):
    groups = own_kv.shape[0]
    per_group = q_ref.shape[1] // groups
    own_rows = q_ref.shape[0]
    fill_ids(n, groups, block_of, outbox)
    for g in range(groups):
        fill_pool(g, n_far, far_owner, far_block, own_kv, gathered_ref, pool_ref)
        attend(g, per_group, chunk_tokens, picked_ref, q_ref, do_ref, dq_ref, pool_ref, acc_ref)
        own_grad[g] = acc_ref[:, :own_rows, :]
        fill_outbox(g, n, own_rows, slot_of, live, block_of, acc_ref, outbox)


def reduce_group(g, n, me, inbox, own_grad, out_ref):
    own_blocks = own_grad.shape[2] // BLK
    dh = own_grad.shape[3]
    base = ID_ROWS + g * 2 * BLK

    def add(k, sums):
        src = lax.rem(me + k, n)
        which = inbox[src, :ID_ROWS, :].astype(jnp.float32)[g : g + 1]
        out = []
        for kv in range(2):
            part = inbox[src, base + kv * BLK : base + (kv + 1) * BLK, :].astype(jnp.float32)
            for b in range(own_blocks):
                out.append(sums[kv * own_blocks + b] + jnp.where(which == float(b), part, 0.0))
        return tuple(out)

    first = tuple(
        own_grad[g, kv, b * BLK : (b + 1) * BLK, :] for kv in range(2) for b in range(own_blocks)
    )
    sums = lax.fori_loop(1, n, add, first)
    for kv in range(2):
        for b in range(own_blocks):
            out_ref[g, kv, b * BLK : (b + 1) * BLK, :] = sums[kv * own_blocks + b].astype(
                jnp.bfloat16
            )


def return_kernel(n, outbox, own_grad, out_ref, inbox, send_sem, recv_sem):
    me = lax.axis_index("ctx")
    barrier_all(n, me)

    def send(k):
        peer = lax.rem(me + k, n)
        return pltpu.make_async_remote_copy(
            src_ref=outbox.at[peer],
            dst_ref=inbox.at[me],
            send_sem=send_sem.at[peer],
            recv_sem=recv_sem.at[me],
            device_id={"ctx": peer},
            device_id_type=pl.DeviceIdType.MESH,
        )

    def arrival(src):
        return pltpu.make_async_remote_copy(
            src_ref=outbox.at[src],
            dst_ref=inbox.at[src],
            send_sem=send_sem.at[src],
            recv_sem=recv_sem.at[src],
            device_id={"ctx": src},
            device_id_type=pl.DeviceIdType.MESH,
        )

    @pl.loop(1, n)
    def _(k):
        send(k).start()

    @pl.loop(1, n)
    def _(k):
        arrival(lax.rem(me + n - k, n)).wait_recv()

    for g in range(own_grad.shape[0]):
        reduce_group(g, n, me, inbox, own_grad, out_ref)

    @pl.loop(1, n)
    def _(k):
        send(k).wait_send()


def tables(selected, tokens, n, fetched):
    own_blocks = tokens // BLK
    me = lax.axis_index("ctx")
    peers = jnp.arange(n, dtype=jnp.int32)
    owner_of = selected // own_blocks
    local_of = selected - owner_of * own_blocks
    match = (owner_of[..., None] == peers) & (peers != me)
    code = jnp.max(jnp.where(match, local_of[..., None] + 1, 0), axis=(0, 2))
    live = (code > 0).astype(jnp.int32)
    block_of = jnp.maximum(code - 1, 0)
    before = (peers[None, :] < peers[:, None]).astype(jnp.int32)
    slot = jnp.sum(before[None] * live[:, None, :], axis=2)
    slot_of = jnp.minimum(slot, fetched - 1)
    pick = (slot[:, None, :] == jnp.arange(fetched)[None, :, None]) & (live[:, None, :] > 0)
    far_owner = jnp.sum(jnp.where(pick, peers, 0), axis=2)
    far_block = jnp.sum(jnp.where(pick, block_of[:, None, :], 0), axis=2)
    far_live = jnp.any(pick, axis=2)
    groups = selected.shape[1]
    own_ids = me * own_blocks + jnp.arange(own_blocks, dtype=jnp.int32)
    far_ids = jnp.where(far_live, far_owner * own_blocks + far_block, -1)
    pool = jnp.concatenate(
        [jnp.broadcast_to(own_ids, (groups, own_blocks)), far_ids], axis=1
    )
    pad = -pool.shape[1] % 16
    pool = jnp.pad(pool, ((0, 0), (0, pad)), constant_values=-1)
    now = me * own_blocks + jnp.arange(tokens, dtype=jnp.int32) // BLK
    chosen = selected.transpose(1, 2, 0)
    picked = jnp.any(chosen[:, None] == pool[:, :, None, None], axis=2)
    picked = picked & (pool[:, :, None] <= now)
    return far_owner, far_block, slot_of, live, block_of, picked.astype(jnp.bfloat16)


def local(queries, keys, values, grad_out, selected):
    tokens, head_count, dh = queries.shape
    groups = keys.shape[1]
    own_blocks = tokens // BLK
    n = lax.axis_size("ctx")
    fetched = min(n - 2, max(selected.shape[2] - own_blocks, 4)) + 1
    pool_rows = (own_blocks + fetched) * BLK
    msg = ID_ROWS + groups * 2 * BLK
    far_owner, far_block, slot_of, live, block_of, picked = tables(selected, tokens, n, fetched)
    own_kv = jnp.stack([keys, values], axis=0).transpose(2, 0, 1, 3)
    any_spec = pl.BlockSpec(memory_space=pl.ANY)
    vmem = pl.BlockSpec(memory_space=pltpu.VMEM)
    smem = pl.BlockSpec(memory_space=pltpu.SMEM)
    gathered = pl.pallas_call(
        functools.partial(gather_kernel, n),
        out_shape=jax.ShapeDtypeStruct((n,) + own_kv.shape, jnp.bfloat16),
        in_specs=[vmem],
        out_specs=vmem,
        scratch_shapes=[
            pltpu.SemaphoreType.DMA((n,)),
            pltpu.SemaphoreType.DMA((n,)),
            pltpu.SemaphoreType.DMA((n,)),
            pltpu.SemaphoreType.DMA,
        ],
        compiler_params=pltpu.CompilerParams(collective_id=0, has_side_effects=True),
    )(own_kv)
    dq, outbox, own_grad = pl.pallas_call(
        functools.partial(attend_kernel, n, fetched, min(tokens, 32)),
        out_shape=(
            jax.ShapeDtypeStruct(queries.shape, jnp.bfloat16),
            jax.ShapeDtypeStruct((n, msg, dh), jnp.bfloat16),
            jax.ShapeDtypeStruct((groups, 2, tokens, dh), jnp.float32),
        ),
        in_specs=[smem] * 5 + [vmem] * 5,
        out_specs=(vmem, vmem, vmem),
        scratch_shapes=[
            pltpu.VMEM((2, pool_rows, dh), jnp.bfloat16),
            pltpu.VMEM((2, pool_rows, dh), jnp.float32),
        ],
    )(far_owner, far_block, slot_of, live, block_of, picked, queries, grad_out, own_kv, gathered)
    summed = pl.pallas_call(
        functools.partial(return_kernel, n),
        out_shape=jax.ShapeDtypeStruct((groups, 2, tokens, dh), jnp.bfloat16),
        in_specs=[vmem, vmem],
        out_specs=vmem,
        scratch_shapes=[
            pltpu.VMEM((n, msg, dh), jnp.bfloat16),
            pltpu.SemaphoreType.DMA((n,)),
            pltpu.SemaphoreType.DMA((n,)),
        ],
        compiler_params=pltpu.CompilerParams(collective_id=1, has_side_effects=True),
    )(outbox, own_grad)
    key_grad = summed[:, 0].transpose(1, 0, 2)
    value_grad = summed[:, 1].transpose(1, 0, 2)
    return dq, key_grad, value_grad


def solution(mesh):
    spec = P(("rep", "ctx"), None, None)
    return jax.shard_map(
        local, mesh=mesh, in_specs=(spec,) * 5, out_specs=(spec,) * 3, check_vma=False
    )
```

```python
import functools
import math

import jax
import jax.numpy as jnp
from jax import lax
from jax.experimental import pallas as pl
from jax.experimental.pallas import tpu as pltpu
from jax.sharding import PartitionSpec as P

BLK = 64
NEG = -1e30
ID_ROWS = 16
LOG2E = math.log2(math.e)
NT = (((1,), (1,)), ((), ()))
NN = (((1,), (0,)), ((), ()))


def barrier_all(n, me):
    barrier = pltpu.get_barrier_semaphore()

    def greet(k, carry):
        peer = lax.rem(me + k, n)
        pl.semaphore_signal(
            barrier, inc=1, device_id={"ctx": peer}, device_id_type=pl.DeviceIdType.MESH
        )
        return carry

    lax.fori_loop(1, n, greet, 0)
    pl.semaphore_wait(barrier, n - 1)


def attend(
    g, per_group, chunk_tokens, lo, hi, picked_ref, q_ref, do_ref, dq_ref, pool_ref, acc_ref
):
    tokens, _, dh = q_ref.shape
    own_rows = tokens
    keys = pool_ref.shape[1]
    slots = keys // BLK
    own_slots = own_rows // BLK
    scaling = 1.0 / math.sqrt(dh)
    log_scale = scaling * LOG2E
    rows = chunk_tokens * per_group
    shift = per_group.bit_length() - 1
    pool_k = pool_ref[0]
    pool_v = pool_ref[1]
    pool_kt = pool_k.T
    heads = slice(g * per_group, (g + 1) * per_group)

    @pl.loop(lo, hi)
    def _(c):
        t0 = pl.multiple_of(c * chunk_tokens, chunk_tokens)
        q = q_ref[pl.ds(t0, chunk_tokens), heads, :].reshape(rows, dh)
        do = do_ref[pl.ds(t0, chunk_tokens), heads, :].reshape(rows, dh)
        row_tok = t0 + (lax.broadcasted_iota(jnp.int32, (tokens, rows), 1) >> shift)
        tok = lax.broadcasted_iota(jnp.int32, (tokens, rows), 0)
        spread = jnp.where(row_tok == tok, 1.0, 0.0).astype(jnp.bfloat16)
        seen = lax.dot_general(picked_ref[g], spread, NN, preferred_element_type=jnp.float32)
        bias = (seen - 1.0) * (-NEG)
        s = lax.dot_general(pool_k, q, NT, preferred_element_type=jnp.float32)
        dp = lax.dot_general(pool_v, do, NT, preferred_element_type=jnp.float32)
        pieces = []
        for j in range(slots):
            piece = s[j * BLK : (j + 1) * BLK] + bias[j : j + 1]
            if j < own_slots:
                key_pos = j * BLK + lax.broadcasted_iota(jnp.int32, (BLK, rows), 0)
                causal = key_pos <= row_tok[:BLK]
                piece = jnp.where(causal, piece, NEG)
            pieces.append(piece)
        s = jnp.concatenate(pieces, axis=0)
        peak = jnp.max(s, axis=0, keepdims=True)
        e = jnp.exp2((s - peak) * log_scale)
        total = jnp.sum(e, axis=0, keepdims=True)
        weighted = jnp.sum(e * dp, axis=0, keepdims=True)
        inv = 1.0 / total
        inner = weighted * inv
        p = e * inv
        ds = (p * (dp - inner)).astype(jnp.bfloat16)
        p = p.astype(jnp.bfloat16)
        dqt = lax.dot_general(pool_kt, ds, NN, preferred_element_type=jnp.float32)
        dq = (dqt * scaling).T.astype(jnp.bfloat16)
        dq_ref[pl.ds(t0, chunk_tokens), heads, :] = dq.reshape(chunk_tokens, per_group, dh)
        dk = lax.dot_general(ds, q, NN, preferred_element_type=jnp.float32)
        dv = lax.dot_general(p, do, NN, preferred_element_type=jnp.float32)
        acc_ref[0] += dk.reshape(slots, BLK, dh)
        acc_ref[1] += dv.reshape(slots, BLK, dh)


def fill_pool(g, n_far, far_owner, far_block, own_kv, gathered_ref, pool_ref):
    own_rows = own_kv.shape[2] * BLK
    pool_ref[:, :own_rows, :] = own_kv[g].reshape(2, own_rows, own_kv.shape[4])
    for s in range(n_far):
        owner = far_owner[g, s]
        block = far_block[g, s]
        lo = own_rows + s * BLK
        for kv in range(2):
            pool_ref[kv, lo : lo + BLK, :] = gathered_ref[owner, kv, block]


def fused_kernel(
    n, cols, n_far, chunk_tokens, groups,
    far_owner, far_block, slot_of, live, block_of,
    picked_ref, q_ref, do_ref, own_kv, dq_ref, out_ref, *scratch,
):
    per_bank = 9
    banks = [scratch[g * per_bank : (g + 1) * per_bank] for g in range(groups)]
    (
        pool_ref, mid_ref, col_send, y_send, sib_send, recv_sem,
        rs_sem, ry_send, ry_recv, rz_send, rz_recv,
    ) = scratch[groups * per_bank :]
    depth = n // (2 * cols)
    chips = n // 2
    me = lax.axis_index("ctx")
    core = lax.rem(me, 2)
    chip = me // 2
    y = lax.rem(chip, cols)
    z = chip // cols
    sib = 2 * chip + 1 - core
    other_y = cols - 1 - y
    y_peer = 2 * (z * cols + other_y) + core
    own_blocks = own_kv.shape[2]
    dh = own_kv.shape[4]
    per_group = q_ref.shape[1] // groups
    chunks = q_ref.shape[0] // chunk_tokens
    scaling = 1.0 / math.sqrt(dh)

    def device(zz, yy, cc):
        return 2 * (zz * cols + yy) + cc

    def remote(src, dst, send, recv, peer):
        return pltpu.make_async_remote_copy(
            src_ref=src,
            dst_ref=dst,
            send_sem=send,
            recv_sem=recv,
            device_id={"ctx": peer},
            device_id_type=pl.DeviceIdType.MESH,
        )

    def col_copy(g, k):
        peer = device(lax.rem(z + k, depth), y, core)
        return remote(
            own_kv.at[g], banks[g][0].at[me], col_send.at[g, k], recv_sem.at[g, me], peer
        )

    def own_copy(g, sem, peer):
        return remote(own_kv.at[g], banks[g][0].at[me], sem, recv_sem.at[g, me], peer)

    def pass_on(g, src, sem, peer):
        slot = banks[g][0].at[src]
        return remote(slot, slot, sem, recv_sem.at[g, src], peer)

    def await_piece(g, src):
        pass_on(g, src, sib_send.at[g, src], sib).wait_recv()

    def gather_start(g):
        if cols > 1:
            own_copy(g, y_send.at[g, z], y_peer).start()

        @pl.loop(1, depth)
        def _(k):
            col_copy(g, k).start()

        own_copy(g, sib_send.at[g, me], sib).start()

    def gather_column(g):
        @pl.loop(1, depth)
        def _(k):
            from_z = lax.rem(z + depth - k, depth)
            src = device(from_z, y, core)
            await_piece(g, src)
            if cols > 1:
                pass_on(g, src, y_send.at[g, from_z], y_peer).start()
            pass_on(g, src, sib_send.at[g, src], sib).start()

    def gather_across(g):
        if cols > 1:
            @pl.loop(0, depth)
            def _(k):
                src = device(lax.rem(z + depth - k, depth), other_y, core)
                await_piece(g, src)
                pass_on(g, src, sib_send.at[g, src], sib).start()

    def gather_end(g):
        @pl.loop(0, chips)
        def _(q):
            await_piece(g, 2 * q + 1 - core)

    def gather_drain(g):
        @pl.loop(1, depth)
        def _(k):
            col_copy(g, k).wait_send()

        if cols > 1:
            @pl.loop(0, depth)
            def _(k):
                pass_on(g, device(k, y, core), y_send.at[g, k], y_peer).wait_send()

        @pl.loop(0, chips)
        def _(q):
            src = 2 * q + core
            pass_on(g, src, sib_send.at[g, src], sib).wait_send()

    def sib_copy(g):
        return remote(banks[g][2], banks[g][3], rs_sem.at[g, 0], rs_sem.at[g, 1], sib)

    def y_copy(g, k):
        return remote(
            banks[g][4].at[k], banks[g][5].at[k], ry_send.at[g, k], ry_recv.at[g, k], y_peer
        )

    def z_copy(g, to_z):
        peer = device(to_z, y, core)
        return remote(
            banks[g][6].at[to_z], banks[g][7].at[z], rz_send.at[g, to_z], rz_recv.at[g, z], peer
        )

    def z_arrival(g, from_z):
        peer = device(from_z, y, core)
        return remote(
            banks[g][6].at[from_z], banks[g][7].at[from_z],
            rz_send.at[g, from_z], rz_recv.at[g, from_z], peer,
        )

    def far_part(g, dest, kv):
        return banks[g][1][kv, own_blocks + slot_of[g, dest]]

    def return_start(g):
        acc_ref, box = banks[g][1], banks[g][2]
        acc_ref[0] = acc_ref[0] * scaling

        @pl.loop(0, chips)
        def _(q):
            dest = 2 * q + 1 - core
            keep = live[g, dest].astype(jnp.float32)
            ids = jnp.full((ID_ROWS, dh), block_of[g, dest].astype(jnp.float32), jnp.float32)
            box[q, :ID_ROWS, :] = ids.astype(jnp.bfloat16)
            for kv in range(2):
                lo = ID_ROWS + kv * BLK
                box[q, lo : lo + BLK, :] = (far_part(g, dest, kv) * keep).astype(jnp.bfloat16)

        sib_copy(g).start()

    def merged(g, zz, yy):
        q = zz * cols + yy
        dest = 2 * q + core
        box = banks[g][3]
        which = box[q, :ID_ROWS, :].astype(jnp.float32)[:1]
        keep = live[g, dest].astype(jnp.float32)
        block = jnp.full((1, dh), block_of[g, dest].astype(jnp.float32), jnp.float32)
        for kv in range(2):
            lo = ID_ROWS + kv * BLK
            theirs = box[q, lo : lo + BLK, :].astype(jnp.float32)
            mine = far_part(g, dest, kv) * keep
            for b in range(own_blocks):
                yield kv, b, (
                    jnp.where(block == float(b), mine, 0.0)
                    + jnp.where(which == float(b), theirs, 0.0)
                )

    def return_across(g):
        sib_copy(g).wait_recv()
        if cols > 1:
            @pl.loop(0, depth)
            def _(k):
                zz = lax.rem(z + 1 + k, depth)
                for kv, b, part in merged(g, zz, other_y):
                    banks[g][4][zz, kv, b] = part.astype(jnp.bfloat16)
                y_copy(g, zz).start()

        @pl.loop(0, depth)
        def _(k):
            for kv, b, part in merged(g, k, y):
                mid_ref[k, kv, b] = part

    def return_column(g):
        @pl.loop(1, depth)
        def _(k):
            to_z = lax.rem(z + k, depth)
            total = mid_ref[to_z]
            if cols > 1:
                y_copy(g, to_z).wait_recv()
                total = total + banks[g][5][to_z].astype(jnp.float32)
            banks[g][6][to_z] = total.astype(jnp.bfloat16)
            z_copy(g, to_z).start()

        total = mid_ref[z] + banks[g][1][:, :own_blocks]
        if cols > 1:
            y_copy(g, z).wait_recv()
            total = total + banks[g][5][z].astype(jnp.float32)
        banks[g][8][...] = total

    def return_end(g):
        @pl.loop(1, depth)
        def _(k):
            from_z = lax.rem(z + depth - k, depth)
            z_arrival(g, from_z).wait_recv()
            banks[g][8][...] += banks[g][7][from_z].astype(jnp.float32)

        out_ref[g] = banks[g][8][...].astype(jnp.bfloat16)

    def return_drain(g):
        sib_copy(g).wait_send()
        if cols > 1:
            @pl.loop(0, depth)
            def _(k):
                y_copy(g, k).wait_send()

        @pl.loop(1, depth)
        def _(k):
            z_copy(g, lax.rem(z + k, depth)).wait_send()

    barrier_all(n, me)
    for g in range(groups):
        gather_start(g)
    for g in range(groups):
        banks[g][1][...] = jnp.zeros_like(banks[g][1])
    gather_column(0)
    gather_across(0)
    gather_end(0)
    for g in range(groups):
        first, last = [], []
        if g + 1 < groups:
            first.append(functools.partial(gather_column, g + 1))
            last.append(functools.partial(gather_across, g + 1))
        if g > 0:
            first.append(functools.partial(return_across, g - 1))
            last.append(functools.partial(return_column, g - 1))
        fill_pool(g, n_far, far_owner, far_block, own_kv, banks[g][0], pool_ref)
        cuts = sorted({0, min(1, chunks), chunks // 2, chunks})
        for i in range(len(cuts) - 1):
            attend(
                g, per_group, chunk_tokens, cuts[i], cuts[i + 1],
                picked_ref, q_ref, do_ref, dq_ref, pool_ref, banks[g][1],
            )
            for step in (first if i == 0 else last if i == len(cuts) - 2 else []):
                step()
        if g + 1 < groups:
            gather_end(g + 1)
        return_start(g)
    final = groups - 1
    return_across(final)
    return_column(final)
    for g in range(groups):
        return_end(g)
    for g in range(groups):
        gather_drain(g)
        return_drain(g)


def columns_of(mesh, n):
    spots = [getattr(d, "coords", None) for d in mesh.devices.reshape(-1, n)[0]]
    if None in spots or n % 2:
        return 1
    cols = sum(spot[2] == spots[0][2] for spot in spots) // 2
    return 2 if cols == 2 and n % 4 == 0 else 1


def tables(selected, tokens, n, fetched):
    own_blocks = tokens // BLK
    me = lax.axis_index("ctx")
    peers = jnp.arange(n, dtype=jnp.int32)
    owner_of = selected // own_blocks
    local_of = selected - owner_of * own_blocks
    match = (owner_of[..., None] == peers) & (peers != me)
    code = jnp.max(jnp.where(match, local_of[..., None] + 1, 0), axis=(0, 2))
    live = (code > 0).astype(jnp.int32)
    block_of = jnp.maximum(code - 1, 0)
    before = (peers[None, :] < peers[:, None]).astype(jnp.int32)
    slot = jnp.sum(before[None] * live[:, None, :], axis=2)
    slot_of = jnp.minimum(slot, fetched - 1)
    pick = (slot[:, None, :] == jnp.arange(fetched)[None, :, None]) & (live[:, None, :] > 0)
    far_owner = jnp.sum(jnp.where(pick, peers, 0), axis=2)
    far_block = jnp.sum(jnp.where(pick, block_of[:, None, :], 0), axis=2)
    far_live = jnp.any(pick, axis=2)
    groups = selected.shape[1]
    own_ids = me * own_blocks + jnp.arange(own_blocks, dtype=jnp.int32)
    far_ids = jnp.where(far_live, far_owner * own_blocks + far_block, -1)
    pool = jnp.concatenate(
        [jnp.broadcast_to(own_ids, (groups, own_blocks)), far_ids], axis=1
    )
    pad = -pool.shape[1] % 16
    pool = jnp.pad(pool, ((0, 0), (0, pad)), constant_values=-1)
    now = me * own_blocks + jnp.arange(tokens, dtype=jnp.int32) // BLK
    chosen = selected.transpose(1, 2, 0)
    picked = jnp.any(chosen[:, None] == pool[:, :, None, None], axis=2)
    picked = picked & (pool[:, :, None] <= now)
    return far_owner, far_block, slot_of, live, block_of, picked.astype(jnp.bfloat16)


def local(cols, queries, keys, values, grad_out, selected):
    tokens, head_count, dh = queries.shape
    groups = keys.shape[1]
    own_blocks = tokens // BLK
    n = lax.axis_size("ctx")
    depth = n // (2 * cols)
    fetched = min(n - 2, max(selected.shape[2] - own_blocks, 4)) + 1
    pool_rows = (own_blocks + fetched) * BLK
    far_owner, far_block, slot_of, live, block_of, picked = tables(selected, tokens, n, fetched)
    own_kv = jnp.stack([keys, values], axis=0).transpose(2, 0, 1, 3)
    piece = (2, own_blocks, BLK, dh)
    own_kv = own_kv.reshape((groups,) + piece)
    vmem = pl.BlockSpec(memory_space=pltpu.VMEM)
    smem = pl.BlockSpec(memory_space=pltpu.SMEM)
    bank = [
        pltpu.VMEM((n,) + piece, jnp.bfloat16),
        pltpu.VMEM((2, pool_rows // BLK, BLK, dh), jnp.float32),
        pltpu.VMEM((n // 2, ID_ROWS + 2 * BLK, dh), jnp.bfloat16),
        pltpu.VMEM((n // 2, ID_ROWS + 2 * BLK, dh), jnp.bfloat16),
        pltpu.VMEM((depth,) + piece, jnp.bfloat16),
        pltpu.VMEM((depth,) + piece, jnp.bfloat16),
        pltpu.VMEM((depth,) + piece, jnp.bfloat16),
        pltpu.VMEM((depth,) + piece, jnp.bfloat16),
        pltpu.VMEM(piece, jnp.float32),
    ]
    dma = pltpu.SemaphoreType.DMA
    dq, summed = pl.pallas_call(
        functools.partial(fused_kernel, n, cols, fetched, min(tokens, 32), groups),
        out_shape=(
            jax.ShapeDtypeStruct(queries.shape, jnp.bfloat16),
            jax.ShapeDtypeStruct((groups,) + piece, jnp.bfloat16),
        ),
        in_specs=[smem] * 5 + [vmem] * 4,
        out_specs=(vmem, vmem),
        scratch_shapes=bank * groups + [
            pltpu.VMEM((2, pool_rows, dh), jnp.bfloat16),
            pltpu.VMEM((depth,) + piece, jnp.float32),
            dma((groups, depth)),
            dma((groups, depth)),
            dma((groups, n)),
            dma((groups, n)),
            dma((groups, 2)),
            dma((groups, depth)),
            dma((groups, depth)),
            dma((groups, depth)),
            dma((groups, depth)),
        ],
        compiler_params=pltpu.CompilerParams(collective_id=0, has_side_effects=True),
    )(far_owner, far_block, slot_of, live, block_of, picked, queries, grad_out, own_kv)
    summed = summed.reshape(groups, 2, tokens, dh)
    key_grad = summed[:, 0].transpose(1, 0, 2)
    value_grad = summed[:, 1].transpose(1, 0, 2)
    return dq, key_grad, value_grad


def solution(mesh):
    spec = P(("rep", "ctx"), None, None)
    cols = columns_of(mesh, mesh.shape["ctx"])
    return jax.shard_map(
        functools.partial(local, cols),
        mesh=mesh,
        in_specs=(spec,) * 5,
        out_specs=(spec,) * 3,
        check_vma=False,
    )
```

```python
import functools
import math

import jax
import jax.numpy as jnp
from jax import lax
from jax.experimental import pallas as pl
from jax.experimental.pallas import tpu as pltpu
from jax.sharding import PartitionSpec as P

BLK = 64
NEG = -1e30
ID_ROWS = 16
LANES = 128
LOG2E = math.log2(math.e)
NT = (((1,), (1,)), ((), ()))
NN = (((1,), (0,)), ((), ()))


def attend(
    g, per_group, chunk_tokens, lo, hi, picked_ref, q_ref, do_ref, dq_ref, pool_ref, acc_ref
):
    tokens, _, dh = q_ref.shape
    own_rows = tokens
    keys = pool_ref.shape[1]
    slots = keys // BLK
    own_slots = own_rows // BLK
    scaling = 1.0 / math.sqrt(dh)
    log_scale = scaling * LOG2E
    rows = chunk_tokens * per_group
    shift = per_group.bit_length() - 1
    pool_k = pool_ref[0]
    pool_v = pool_ref[1]
    pool_kt = pool_k.T
    heads = slice(g * per_group, (g + 1) * per_group)

    @pl.loop(lo, hi)
    def _(c):
        t0 = pl.multiple_of(c * chunk_tokens, chunk_tokens)
        q = q_ref[pl.ds(t0, chunk_tokens), heads, :].reshape(rows, dh)
        do = do_ref[pl.ds(t0, chunk_tokens), heads, :].reshape(rows, dh)
        row_tok = t0 + (lax.broadcasted_iota(jnp.int32, (tokens, rows), 1) >> shift)
        tok = lax.broadcasted_iota(jnp.int32, (tokens, rows), 0)
        spread = jnp.where(row_tok == tok, 1.0, 0.0).astype(jnp.bfloat16)
        seen = lax.dot_general(picked_ref[g], spread, NN, preferred_element_type=jnp.float32)
        bias = (seen - 1.0) * (-NEG)
        s = lax.dot_general(pool_k, q, NT, preferred_element_type=jnp.float32)
        dp = lax.dot_general(pool_v, do, NT, preferred_element_type=jnp.float32)
        pieces = []
        for j in range(slots):
            piece = s[j * BLK : (j + 1) * BLK] + bias[j : j + 1]
            if j < own_slots:
                key_pos = j * BLK + lax.broadcasted_iota(jnp.int32, (BLK, rows), 0)
                causal = key_pos <= row_tok[:BLK]
                piece = jnp.where(causal, piece, NEG)
            pieces.append(piece)
        s = jnp.concatenate(pieces, axis=0)
        peak = jnp.max(s, axis=0, keepdims=True)
        e = jnp.exp2((s - peak) * log_scale)
        total = jnp.sum(e, axis=0, keepdims=True)
        weighted = jnp.sum(e * dp, axis=0, keepdims=True)
        inv = 1.0 / total
        inner = weighted * inv
        p = e * inv
        ds = (p * (dp - inner)).astype(jnp.bfloat16)
        p = p.astype(jnp.bfloat16)
        dqt = lax.dot_general(pool_kt, ds, NN, preferred_element_type=jnp.float32)
        dq = (dqt * scaling).T.astype(jnp.bfloat16)
        dq_ref[pl.ds(t0, chunk_tokens), heads, :] = dq.reshape(chunk_tokens, per_group, dh)
        dk = lax.dot_general(ds, q, NN, preferred_element_type=jnp.float32)
        dv = lax.dot_general(p, do, NN, preferred_element_type=jnp.float32)
        acc_ref[0] += dk.reshape(slots, BLK, dh)
        acc_ref[1] += dv.reshape(slots, BLK, dh)


def fill_tables(g, n, me, n_far, own_blocks, sel_ref, picked_ref, tab_ref):
    sel = sel_ref[g]
    tokens = sel.shape[1]
    shift = own_blocks.bit_length() - 1
    owner = sel >> shift
    block = sel & (own_blocks - 1)
    peers = lax.broadcasted_iota(jnp.int32, (n, tokens), 0)
    code = jnp.zeros((n, tokens), jnp.float32)
    for i in range(sel.shape[0]):
        mark = (block[i : i + 1] + 1).astype(jnp.float32)
        code = jnp.maximum(code, jnp.where(owner[i : i + 1] == peers, mark, 0.0))
    code = jnp.broadcast_to(jnp.max(code, axis=1, keepdims=True), (n, LANES))
    peers = lax.broadcasted_iota(jnp.int32, (n, LANES), 0)
    code = jnp.where(peers == me, 0.0, code)
    live = jnp.where(code > 0.0, 1.0, 0.0)
    before = lax.broadcasted_iota(jnp.int32, (n, n), 1) < lax.broadcasted_iota(jnp.int32, (n, n), 0)
    before = jnp.where(before, 1.0, 0.0).astype(jnp.bfloat16)
    slot = lax.dot_general(before, live.astype(jnp.bfloat16), NN, preferred_element_type=jnp.float32)
    far = jnp.maximum(code - 1.0, 0.0)
    lane = lax.broadcasted_iota(jnp.int32, (n, LANES), 1)
    kept = jnp.minimum(slot, float(n_far - 1))
    entry = jnp.where(lane == 0, kept, jnp.where(lane == 1, live, far))
    tab_ref[g, :n, :] = entry.astype(jnp.int32)
    peer = peers.astype(jnp.float32)
    now = me * own_blocks + (lax.broadcasted_iota(jnp.int32, (1, tokens), 1) >> BLK.bit_length() - 1)
    slots = picked_ref.shape[1]
    row = lax.broadcasted_iota(jnp.int32, (slots, tokens), 0)
    far_rows = tab_ref.shape[1] - n
    far_row = lax.broadcasted_iota(jnp.int32, (far_rows, LANES), 0)
    far_lane = lax.broadcasted_iota(jnp.int32, (far_rows, LANES), 1)
    far_entry = jnp.zeros((far_rows, LANES), jnp.float32)
    picked = jnp.zeros((slots, tokens), jnp.float32)
    for i in range(own_blocks + n_far):
        if i < own_blocks:
            ids = jnp.full((1, tokens), me * own_blocks + i, jnp.int32)
        else:
            hit = (live > 0.0) & (slot == float(i - own_blocks))
            who = jnp.max(jnp.where(hit, peer, -1.0), axis=0, keepdims=True)
            which = jnp.max(jnp.where(hit, far, 0.0), axis=0, keepdims=True)
            ids = jnp.max(who * own_blocks + which, axis=1, keepdims=True).astype(jnp.int32)
            ids = jnp.broadcast_to(ids, (1, tokens))
            here = jnp.where(far_lane == 0, jnp.maximum(who, 0.0), which)
            far_entry = jnp.where(far_row == i - own_blocks, here, far_entry)
        seen = jnp.max(jnp.where(sel == ids, 1.0, 0.0), axis=0, keepdims=True)
        seen = jnp.where(ids <= now, seen, 0.0)
        picked = jnp.where(row == i, seen, picked)
    tab_ref[g, n:, :] = far_entry.astype(jnp.int32)
    picked_ref[g] = picked.astype(jnp.bfloat16)


def fill_pool(g, n, n_far, tab, own_kv, gathered_ref, pool_ref):
    own_rows = own_kv.shape[2] * BLK
    pool_ref[:, :own_rows, :] = own_kv[g].reshape(2, own_rows, own_kv.shape[4])
    for s in range(n_far):
        owner = jnp.clip(tab[g, n + s, 0], 0, n - 1)
        block = jnp.clip(tab[g, n + s, 1], 0, own_kv.shape[2] - 1)
        lo = own_rows + s * BLK
        for kv in range(2):
            pool_ref[kv, lo : lo + BLK, :] = gathered_ref[owner, kv, block]


def fused_kernel(
    n, cols, n_far, chunk_tokens, groups,
    sel_ref, q_hbm, do_hbm, own_kv, dq_ref, key_out, value_out, *scratch,
):
    per_bank = 9
    banks = [scratch[g * per_bank : (g + 1) * per_bank] for g in range(groups)]
    (
        picked_ref, tab_ref, tab, q_ref, do_ref, mix_ref, in_sem, pool_ref, mid_ref, col_send, y_send, sib_send, recv_sem,
        rs_sem, ry_send, ry_recv, rz_send, rz_recv,
    ) = scratch[groups * per_bank :]
    depth = n // (2 * cols)
    chips = n // 2
    me = lax.axis_index("ctx")
    core = lax.rem(me, 2)
    chip = me // 2
    y = lax.rem(chip, cols)
    z = chip // cols
    sib = 2 * chip + 1 - core
    other_y = cols - 1 - y
    y_peer = 2 * (z * cols + other_y) + core
    own_blocks = own_kv.shape[2]
    own_rows = own_blocks * BLK
    dh = own_kv.shape[4]
    per_group = q_ref.shape[1] // groups
    chunks = q_ref.shape[0] // chunk_tokens
    scaling = 1.0 / math.sqrt(dh)

    def device(zz, yy, cc):
        return 2 * (zz * cols + yy) + cc

    def remote(src, dst, send, recv, peer):
        return pltpu.make_async_remote_copy(
            src_ref=src,
            dst_ref=dst,
            send_sem=send,
            recv_sem=recv,
            device_id={"ctx": peer},
            device_id_type=pl.DeviceIdType.MESH,
        )

    def col_copy(g, k):
        peer = device(lax.rem(z + k, depth), y, core)
        return remote(
            own_kv.at[g], banks[g][0].at[me], col_send.at[g, k], recv_sem.at[g, me], peer
        )

    def own_copy(g, sem, peer):
        return remote(own_kv.at[g], banks[g][0].at[me], sem, recv_sem.at[g, me], peer)

    def pass_on(g, src, sem, peer):
        slot = banks[g][0].at[src]
        return remote(slot, slot, sem, recv_sem.at[g, src], peer)

    def await_piece(g, src):
        pass_on(g, src, sib_send.at[g, src], sib).wait_recv()

    def gather_start(g):
        if cols > 1:
            own_copy(g, y_send.at[g, z], y_peer).start()

        @pl.loop(1, depth)
        def _(k):
            col_copy(g, k).start()

        own_copy(g, sib_send.at[g, me], sib).start()

    def gather_column(g):
        @pl.loop(1, depth)
        def _(k):
            from_z = lax.rem(z + depth - k, depth)
            src = device(from_z, y, core)
            await_piece(g, src)
            if cols > 1:
                pass_on(g, src, y_send.at[g, from_z], y_peer).start()
            pass_on(g, src, sib_send.at[g, src], sib).start()

    def gather_across(g):
        if cols > 1:
            @pl.loop(0, depth)
            def _(k):
                src = device(lax.rem(z + depth - k, depth), other_y, core)
                await_piece(g, src)
                pass_on(g, src, sib_send.at[g, src], sib).start()

    def gather_end(g):
        @pl.loop(0, chips)
        def _(q):
            await_piece(g, 2 * q + 1 - core)

    def gather_drain(g):
        @pl.loop(1, depth)
        def _(k):
            col_copy(g, k).wait_send()

        if cols > 1:
            @pl.loop(0, depth)
            def _(k):
                pass_on(g, device(k, y, core), y_send.at[g, k], y_peer).wait_send()

        @pl.loop(0, chips)
        def _(q):
            src = 2 * q + core
            pass_on(g, src, sib_send.at[g, src], sib).wait_send()

    def sib_copy(g):
        return remote(banks[g][2], banks[g][3], rs_sem.at[g, 0], rs_sem.at[g, 1], sib)

    def y_copy(g, k):
        return remote(
            banks[g][4].at[k], banks[g][5].at[k], ry_send.at[g, k], ry_recv.at[g, k], y_peer
        )

    def z_copy(g, to_z):
        peer = device(to_z, y, core)
        return remote(
            banks[g][6].at[to_z], banks[g][7].at[z], rz_send.at[g, to_z], rz_recv.at[g, z], peer
        )

    def z_arrival(g, from_z):
        peer = device(from_z, y, core)
        return remote(
            banks[g][6].at[from_z], banks[g][7].at[from_z],
            rz_send.at[g, from_z], rz_recv.at[g, from_z], peer,
        )

    def far_part(g, dest, kv):
        return banks[g][1][kv, own_blocks + jnp.clip(tab[g, dest, 0], 0, n_far - 1)]

    def return_start(g):
        acc_ref, box = banks[g][1], banks[g][2]
        acc_ref[0] = acc_ref[0] * scaling

        @pl.loop(0, chips)
        def _(q):
            dest = 2 * q + 1 - core
            keep = tab[g, dest, 1].astype(jnp.float32)
            ids = jnp.full((ID_ROWS, dh), tab[g, dest, 2].astype(jnp.float32), jnp.float32)
            box[q, :ID_ROWS, :] = ids.astype(jnp.bfloat16)
            for kv in range(2):
                lo = ID_ROWS + kv * BLK
                box[q, lo : lo + BLK, :] = (far_part(g, dest, kv) * keep).astype(jnp.bfloat16)

        sib_copy(g).start()

    def merged(g, zz, yy):
        q = zz * cols + yy
        dest = 2 * q + core
        box = banks[g][3]
        which = box[q, :ID_ROWS, :].astype(jnp.float32)[:1]
        keep = tab[g, dest, 1].astype(jnp.float32)
        block = jnp.full((1, dh), tab[g, dest, 2].astype(jnp.float32), jnp.float32)
        for kv in range(2):
            lo = ID_ROWS + kv * BLK
            theirs = box[q, lo : lo + BLK, :].astype(jnp.float32)
            mine = far_part(g, dest, kv) * keep
            for b in range(own_blocks):
                yield kv, b, (
                    jnp.where(block == float(b), mine, 0.0)
                    + jnp.where(which == float(b), theirs, 0.0)
                )

    def return_across(g):
        sib_copy(g).wait_recv()
        if cols > 1:
            @pl.loop(0, depth)
            def _(k):
                zz = lax.rem(z + 1 + k, depth)
                for kv, b, part in merged(g, zz, other_y):
                    banks[g][4][zz, kv, b] = part.astype(jnp.bfloat16)
                y_copy(g, zz).start()

        @pl.loop(0, depth)
        def _(k):
            for kv, b, part in merged(g, k, y):
                mid_ref[k, kv, b] = part

    def return_column(g):
        @pl.loop(1, depth)
        def _(k):
            to_z = lax.rem(z + k, depth)
            total = mid_ref[to_z]
            if cols > 1:
                y_copy(g, to_z).wait_recv()
                total = total + banks[g][5][to_z].astype(jnp.float32)
            banks[g][6][to_z] = total.astype(jnp.bfloat16)
            z_copy(g, to_z).start()

        total = mid_ref[z] + banks[g][1][:, :own_blocks]
        if cols > 1:
            y_copy(g, z).wait_recv()
            total = total + banks[g][5][z].astype(jnp.float32)
        banks[g][8][...] = total

    def return_end(g):
        @pl.loop(1, depth)
        def _(k):
            from_z = lax.rem(z + depth - k, depth)
            z_arrival(g, from_z).wait_recv()
            banks[g][8][...] += banks[g][7][from_z].astype(jnp.float32)

        for kv in range(2):
            whole = banks[g][8][kv].reshape(own_rows, dh)
            mix_ref[kv, pl.ds(g, own_rows, stride=groups), :] = whole

    def return_drain(g):
        sib_copy(g).wait_send()
        if cols > 1:
            @pl.loop(0, depth)
            def _(k):
                y_copy(g, k).wait_send()

        @pl.loop(1, depth)
        def _(k):
            z_copy(g, lax.rem(z + k, depth)).wait_send()

    barrier = pltpu.get_barrier_semaphore()

    def greet(peer):
        pl.semaphore_signal(
            barrier, inc=1, device_id={"ctx": peer}, device_id_type=pl.DeviceIdType.MESH
        )

    @pl.loop(1, depth)
    def _(k):
        greet(device(lax.rem(z + k, depth), y, core))

    if cols > 1:
        greet(y_peer)
    greet(sib)
    loads = [
        pltpu.make_async_copy(q_hbm, q_ref, in_sem.at[0]),
        pltpu.make_async_copy(do_hbm, do_ref, in_sem.at[1]),
    ]
    for load in loads:
        load.start()
    pl.semaphore_wait(barrier, depth + cols - 1)
    for g in range(groups):
        gather_start(g)
    for g in range(groups):
        fill_tables(g, n, me, n_far, own_blocks, sel_ref, picked_ref, tab_ref)
    to_scalars = pltpu.make_async_copy(tab_ref, tab, in_sem.at[2])
    to_scalars.start()
    for g in range(groups):
        banks[g][1][...] = jnp.zeros_like(banks[g][1])
    to_scalars.wait()
    for load in loads:
        load.wait()
    gather_column(0)
    gather_across(0)
    gather_end(0)
    for g in range(groups):
        first, last = [], []
        if g + 1 < groups:
            first.append(functools.partial(gather_column, g + 1))
            last.append(functools.partial(gather_across, g + 1))
        if g > 0:
            first.append(functools.partial(return_across, g - 1))
            last.append(functools.partial(return_column, g - 1))
        fill_pool(g, n, n_far, tab, own_kv, banks[g][0], pool_ref)
        cuts = sorted({0, min(1, chunks), chunks // 2, chunks})
        for i in range(len(cuts) - 1):
            attend(
                g, per_group, chunk_tokens, cuts[i], cuts[i + 1],
                picked_ref, q_ref, do_ref, dq_ref, pool_ref, banks[g][1],
            )
            for step in (first if i == 0 else last if i == len(cuts) - 2 else []):
                step()
        if g + 1 < groups:
            gather_end(g + 1)
        return_start(g)
    final = groups - 1
    return_across(final)
    return_column(final)
    for g in range(groups):
        return_end(g)
    for g in range(groups):
        gather_drain(g)
        return_drain(g)
    key_out[...] = mix_ref[0, : own_rows * groups].astype(jnp.bfloat16)
    value_out[...] = mix_ref[1, : own_rows * groups].astype(jnp.bfloat16)


def columns_of(mesh, n):
    spots = [getattr(d, "coords", None) for d in mesh.devices.reshape(-1, n)[0]]
    if None in spots or n % 2:
        return 1
    cols = sum(spot[2] == spots[0][2] for spot in spots) // 2
    return 2 if cols == 2 and n % 4 == 0 else 1


def local(cols, queries, keys, values, grad_out, selected):
    tokens, head_count, dh = queries.shape
    groups = keys.shape[1]
    own_blocks = tokens // BLK
    n = lax.axis_size("ctx")
    depth = n // (2 * cols)
    fetched = min(n - 2, max(selected.shape[2] - own_blocks, 4)) + 1
    slots = -(-(own_blocks + fetched) // 16) * 16
    far_rows = -(-fetched // 8) * 8
    pool_rows = (own_blocks + fetched) * BLK
    chosen = selected.transpose(1, 2, 0)
    own_kv = jnp.stack([keys, values], axis=0).transpose(2, 0, 1, 3)
    piece = (2, own_blocks, BLK, dh)
    own_kv = own_kv.reshape((groups,) + piece)
    vmem = pl.BlockSpec(memory_space=pltpu.VMEM)
    any_spec = pl.BlockSpec(memory_space=pl.ANY)
    bank = [
        pltpu.VMEM((n,) + piece, jnp.bfloat16),
        pltpu.VMEM((2, pool_rows // BLK, BLK, dh), jnp.float32),
        pltpu.VMEM((n // 2, ID_ROWS + 2 * BLK, dh), jnp.bfloat16),
        pltpu.VMEM((n // 2, ID_ROWS + 2 * BLK, dh), jnp.bfloat16),
        pltpu.VMEM((depth,) + piece, jnp.bfloat16),
        pltpu.VMEM((depth,) + piece, jnp.bfloat16),
        pltpu.VMEM((depth,) + piece, jnp.bfloat16),
        pltpu.VMEM((depth,) + piece, jnp.bfloat16),
        pltpu.VMEM(piece, jnp.float32),
    ]
    dma = pltpu.SemaphoreType.DMA
    dq, key_grad, value_grad = pl.pallas_call(
        functools.partial(fused_kernel, n, cols, fetched, min(tokens, 32), groups),
        out_shape=(
            jax.ShapeDtypeStruct(queries.shape, jnp.bfloat16),
            jax.ShapeDtypeStruct((tokens * groups, dh), jnp.bfloat16),
            jax.ShapeDtypeStruct((tokens * groups, dh), jnp.bfloat16),
        ),
        in_specs=[vmem, any_spec, any_spec, vmem],
        out_specs=(vmem, vmem, vmem),
        scratch_shapes=bank * groups + [
            pltpu.VMEM((groups, slots, tokens), jnp.bfloat16),
            pltpu.VMEM((groups, n + far_rows, LANES), jnp.int32),
            pltpu.SMEM((groups, n + far_rows, LANES), jnp.int32),
            pltpu.VMEM(queries.shape, jnp.bfloat16),
            pltpu.VMEM(queries.shape, jnp.bfloat16),
            pltpu.VMEM((2, tokens * groups + 8, dh), jnp.float32),
            dma((3,)),
            pltpu.VMEM((2, pool_rows, dh), jnp.bfloat16),
            pltpu.VMEM((depth,) + piece, jnp.float32),
            dma((groups, depth)),
            dma((groups, depth)),
            dma((groups, n)),
            dma((groups, n)),
            dma((groups, 2)),
            dma((groups, depth)),
            dma((groups, depth)),
            dma((groups, depth)),
            dma((groups, depth)),
        ],
        compiler_params=pltpu.CompilerParams(collective_id=0, has_side_effects=True),
    )(chosen, queries, grad_out, own_kv)
    return dq, key_grad.reshape(keys.shape), value_grad.reshape(values.shape)


def solution(mesh):
    spec = P(("rep", "ctx"), None, None)
    cols = columns_of(mesh, mesh.shape["ctx"])
    return jax.shard_map(
        functools.partial(local, cols),
        mesh=mesh,
        in_specs=(spec,) * 5,
        out_specs=(spec,) * 3,
        check_vma=False,
    )
```

```python
import functools
import math

import jax
import jax.numpy as jnp
from jax import lax
from jax.experimental import pallas as pl
from jax.experimental.pallas import tpu as pltpu
from jax.sharding import PartitionSpec as P

BLK = 64
NEG = -1e30
ID_ROWS = 16
LANES = 128
LOG2E = math.log2(math.e)
NT = (((1,), (1,)), ((), ()))
NN = (((1,), (0,)), ((), ()))


def weigh(g, per_group, chunk, chunk_tokens, own_slots, picked_ref, q_ref, do_ref, pool_ref, p_ref, acc_ref):
    tokens, _, dh = q_ref.shape
    keys = pool_ref.shape[1]
    slots = keys // BLK
    log_scale = LOG2E / math.sqrt(dh)
    rows = chunk_tokens * per_group
    shift = per_group.bit_length() - 1
    heads = slice(g * per_group, (g + 1) * per_group)
    t0 = chunk * chunk_tokens
    q = q_ref[t0 : t0 + chunk_tokens, heads, :].reshape(rows, dh)
    do = do_ref[t0 : t0 + chunk_tokens, heads, :].reshape(rows, dh)
    row_tok = t0 + (lax.broadcasted_iota(jnp.int32, (tokens, rows), 1) >> shift)
    tok = lax.broadcasted_iota(jnp.int32, (tokens, rows), 0)
    spread = jnp.where(row_tok == tok, 1.0, 0.0).astype(jnp.bfloat16)
    seen = lax.dot_general(picked_ref[g], spread, NN, preferred_element_type=jnp.float32)
    bias = (seen - 1.0) * (-NEG)
    s = lax.dot_general(pool_ref[0], q, NT, preferred_element_type=jnp.float32)
    pieces = []
    for j in range(slots):
        piece = s[j * BLK : (j + 1) * BLK] + bias[j : j + 1]
        if j < own_slots:
            key_pos = j * BLK + lax.broadcasted_iota(jnp.int32, (BLK, rows), 0)
            piece = jnp.where(key_pos <= row_tok[:BLK], piece, NEG)
        pieces.append(piece)
    s = jnp.concatenate(pieces, axis=0)
    peak = jnp.max(s, axis=0, keepdims=True)
    e = jnp.exp2((s - peak) * log_scale)
    p = e * (1.0 / jnp.sum(e, axis=0, keepdims=True))
    p_ref[chunk] = p
    dv = lax.dot_general(p.astype(jnp.bfloat16), do, NN, preferred_element_type=jnp.float32)
    dv = dv.reshape(slots, BLK, dh)
    acc_ref[...] = dv if chunk == 0 else acc_ref[...] + dv


def differentiate(g, per_group, chunk, chunk_tokens, q_ref, do_ref, dq_ref, pool_ref, p_ref, acc_ref):
    dh = q_ref.shape[2]
    keys = pool_ref.shape[1]
    scaling = 1.0 / math.sqrt(dh)
    rows = chunk_tokens * per_group
    heads = slice(g * per_group, (g + 1) * per_group)
    t0 = chunk * chunk_tokens
    q = q_ref[t0 : t0 + chunk_tokens, heads, :].reshape(rows, dh)
    do = do_ref[t0 : t0 + chunk_tokens, heads, :].reshape(rows, dh)
    p = p_ref[chunk]
    dp = lax.dot_general(pool_ref[1], do, NT, preferred_element_type=jnp.float32)
    inner = jnp.sum(p * dp, axis=0, keepdims=True)
    ds = (p * (dp - inner)).astype(jnp.bfloat16)
    dqt = lax.dot_general(pool_ref[0].T, ds, NN, preferred_element_type=jnp.float32)
    dq = (dqt * scaling).T.astype(jnp.bfloat16)
    dq_ref[t0 : t0 + chunk_tokens, heads, :] = dq.reshape(chunk_tokens, per_group, dh)
    dk = lax.dot_general(ds, q, NN, preferred_element_type=jnp.float32)
    dk = dk.reshape(keys // BLK, BLK, dh)
    acc_ref[...] = dk if chunk == 0 else acc_ref[...] + dk


def fill_tables(g, n, me, n_far, own_blocks, sel_ref, picked_ref, tab_ref):
    sel = sel_ref[g]
    tokens = sel.shape[1]
    shift = own_blocks.bit_length() - 1
    owner = sel >> shift
    block = sel & (own_blocks - 1)
    peers = lax.broadcasted_iota(jnp.int32, (n, tokens), 0)
    code = jnp.zeros((n, tokens), jnp.float32)
    for i in range(sel.shape[0]):
        mark = (block[i : i + 1] + 1).astype(jnp.float32)
        code = jnp.maximum(code, jnp.where(owner[i : i + 1] == peers, mark, 0.0))
    code = jnp.broadcast_to(jnp.max(code, axis=1, keepdims=True), (n, LANES))
    peers = lax.broadcasted_iota(jnp.int32, (n, LANES), 0)
    code = jnp.where(peers == me, 0.0, code)
    live = jnp.where(code > 0.0, 1.0, 0.0)
    before = lax.broadcasted_iota(jnp.int32, (n, n), 1) < lax.broadcasted_iota(jnp.int32, (n, n), 0)
    before = jnp.where(before, 1.0, 0.0).astype(jnp.bfloat16)
    slot = lax.dot_general(before, live.astype(jnp.bfloat16), NN, preferred_element_type=jnp.float32)
    far = jnp.maximum(code - 1.0, 0.0)
    lane = lax.broadcasted_iota(jnp.int32, (n, LANES), 1)
    kept = jnp.minimum(slot, float(n_far - 1))
    entry = jnp.where(lane == 0, kept, jnp.where(lane == 1, live, far))
    tab_ref[g, :n, :] = entry.astype(jnp.int32)
    peer = peers.astype(jnp.float32)
    now = me * own_blocks + (lax.broadcasted_iota(jnp.int32, (1, tokens), 1) >> BLK.bit_length() - 1)
    slots = picked_ref.shape[1]
    row = lax.broadcasted_iota(jnp.int32, (slots, tokens), 0)
    far_rows = tab_ref.shape[1] - n
    far_row = lax.broadcasted_iota(jnp.int32, (far_rows, LANES), 0)
    far_lane = lax.broadcasted_iota(jnp.int32, (far_rows, LANES), 1)
    far_entry = jnp.zeros((far_rows, LANES), jnp.float32)
    picked = jnp.zeros((slots, tokens), jnp.float32)
    for i in range(own_blocks + n_far):
        if i < own_blocks:
            ids = jnp.full((1, tokens), me * own_blocks + i, jnp.int32)
        else:
            hit = (live > 0.0) & (slot == float(i - own_blocks))
            who = jnp.max(jnp.where(hit, peer, -1.0), axis=0, keepdims=True)
            which = jnp.max(jnp.where(hit, far, 0.0), axis=0, keepdims=True)
            ids = jnp.max(who * own_blocks + which, axis=1, keepdims=True).astype(jnp.int32)
            ids = jnp.broadcast_to(ids, (1, tokens))
            here = jnp.where(far_lane == 0, jnp.maximum(who, 0.0), which)
            far_entry = jnp.where(far_row == i - own_blocks, here, far_entry)
        seen = jnp.max(jnp.where(sel == ids, 1.0, 0.0), axis=0, keepdims=True)
        seen = jnp.where(ids <= now, seen, 0.0)
        picked = jnp.where(row == i, seen, picked)
    tab_ref[g, n:, :] = far_entry.astype(jnp.int32)
    picked_ref[g] = picked.astype(jnp.bfloat16)


def fill_pool(unit, n, n_far, tab, own_kv, gathered_ref, pool_ref):
    group, kv = divmod(unit, 2)
    own_blocks = own_kv.shape[1]
    own_rows = own_blocks * BLK
    pool_ref[kv, :own_rows, :] = own_kv[unit].reshape(own_rows, own_kv.shape[3])
    for s in range(n_far):
        owner = jnp.clip(tab[group, n + s, 0], 0, n - 1)
        block = jnp.clip(tab[group, n + s, 1], 0, own_blocks - 1)
        lo = own_rows + s * BLK
        pool_ref[kv, lo : lo + BLK, :] = gathered_ref[owner, block]


def fused_kernel(
    n, cols, n_far, chunk_tokens, groups,
    sel_ref, q_hbm, do_hbm, own_kv, dq_ref, key_out, value_out, *scratch,
):
    per_bank = 10
    units = 2 * groups
    banks = [scratch[g * per_bank : (g + 1) * per_bank] for g in range(units)]
    (
        picked_ref, tab_ref, tab, q_ref, do_ref, mix_ref, in_sem, pool_ref, p_ref, col_send, y_send, sib_send, recv_sem,
        rs_sem, ry_send, ry_recv, rz_send, rz_recv,
    ) = scratch[units * per_bank :]
    depth = n // (2 * cols)
    chips = n // 2
    me = lax.axis_index("ctx")
    core = lax.rem(me, 2)
    chip = me // 2
    y = lax.rem(chip, cols)
    z = chip // cols
    sib = 2 * chip + 1 - core
    other_y = cols - 1 - y
    y_peer = 2 * (z * cols + other_y) + core
    own_blocks = own_kv.shape[1]
    own_rows = own_blocks * BLK
    dh = own_kv.shape[3]
    per_group = q_ref.shape[1] // groups
    chunks = q_ref.shape[0] // chunk_tokens
    scaling = 1.0 / math.sqrt(dh)

    def device(zz, yy, cc):
        return 2 * (zz * cols + yy) + cc

    def remote(src, dst, send, recv, peer):
        return pltpu.make_async_remote_copy(
            src_ref=src,
            dst_ref=dst,
            send_sem=send,
            recv_sem=recv,
            device_id={"ctx": peer},
            device_id_type=pl.DeviceIdType.MESH,
        )

    def col_copy(g, k):
        peer = device(lax.rem(z + k, depth), y, core)
        return remote(
            own_kv.at[g], banks[g][0].at[me], col_send.at[g, k], recv_sem.at[g, me], peer
        )

    def own_copy(g, sem, peer):
        return remote(own_kv.at[g], banks[g][0].at[me], sem, recv_sem.at[g, me], peer)

    def pass_on(g, src, sem, peer):
        slot = banks[g][0].at[src]
        return remote(slot, slot, sem, recv_sem.at[g, src], peer)

    def await_piece(g, src):
        pass_on(g, src, sib_send.at[g, src], sib).wait_recv()

    def gather_start(g):
        if cols > 1:
            own_copy(g, y_send.at[g, z], y_peer).start()

        @pl.loop(1, depth)
        def _(k):
            col_copy(g, k).start()

        own_copy(g, sib_send.at[g, me], sib).start()

    def gather_column(g):
        @pl.loop(1, depth)
        def _(k):
            from_z = lax.rem(z + depth - k, depth)
            src = device(from_z, y, core)
            await_piece(g, src)
            if cols > 1:
                pass_on(g, src, y_send.at[g, from_z], y_peer).start()
            pass_on(g, src, sib_send.at[g, src], sib).start()

    def gather_across(g):
        if cols > 1:
            @pl.loop(0, depth)
            def _(k):
                src = device(lax.rem(z + depth - k, depth), other_y, core)
                await_piece(g, src)
                pass_on(g, src, sib_send.at[g, src], sib).start()

    def gather_end(g):
        @pl.loop(0, chips)
        def _(q):
            await_piece(g, 2 * q + 1 - core)

    def gather_drain(g):
        @pl.loop(1, depth)
        def _(k):
            col_copy(g, k).wait_send()

        if cols > 1:
            @pl.loop(0, depth)
            def _(k):
                pass_on(g, device(k, y, core), y_send.at[g, k], y_peer).wait_send()

        @pl.loop(0, chips)
        def _(q):
            src = 2 * q + core
            pass_on(g, src, sib_send.at[g, src], sib).wait_send()

    def sib_copy(g):
        return remote(banks[g][2], banks[g][3], rs_sem.at[g, 0], rs_sem.at[g, 1], sib)

    def y_copy(g, k):
        return remote(
            banks[g][4].at[k], banks[g][5].at[k], ry_send.at[g, k], ry_recv.at[g, k], y_peer
        )

    def z_copy(g, to_z):
        peer = device(to_z, y, core)
        return remote(
            banks[g][6].at[to_z], banks[g][7].at[z], rz_send.at[g, to_z], rz_recv.at[g, z], peer
        )

    def z_arrival(g, from_z):
        peer = device(from_z, y, core)
        return remote(
            banks[g][6].at[from_z], banks[g][7].at[from_z],
            rz_send.at[g, from_z], rz_recv.at[g, from_z], peer,
        )

    def far_part(g, dest):
        return banks[g][1][own_blocks + jnp.clip(tab[g // 2, dest, 0], 0, n_far - 1)]

    def return_start(g):
        acc_ref, box = banks[g][1], banks[g][2]
        if g % 2 == 0:
            acc_ref[...] = acc_ref[...] * scaling

        @pl.loop(0, chips)
        def _(q):
            dest = 2 * q + 1 - core
            keep = tab[g // 2, dest, 1].astype(jnp.float32)
            block = tab[g // 2, dest, 2].astype(jnp.float32)
            box[q, :ID_ROWS, :] = jnp.full((ID_ROWS, dh), block, jnp.float32).astype(jnp.bfloat16)
            box[q, ID_ROWS:, :] = (far_part(g, dest) * keep).astype(jnp.bfloat16)

        sib_copy(g).start()

    def merged(g, zz, yy):
        q = zz * cols + yy
        dest = 2 * q + core
        box = banks[g][3]
        which = box[q, :ID_ROWS, :].astype(jnp.float32)[:1]
        keep = tab[g // 2, dest, 1].astype(jnp.float32)
        block = jnp.full((1, dh), tab[g // 2, dest, 2].astype(jnp.float32), jnp.float32)
        theirs = box[q, ID_ROWS:, :].astype(jnp.float32)
        mine = far_part(g, dest) * keep
        for b in range(own_blocks):
            yield b, (
                jnp.where(block == float(b), mine, 0.0) + jnp.where(which == float(b), theirs, 0.0)
            )

    def return_across(g):
        sib_copy(g).wait_recv()
        if cols > 1:
            @pl.loop(0, depth)
            def _(k):
                zz = lax.rem(z + 1 + k, depth)
                for b, part in merged(g, zz, other_y):
                    banks[g][4][zz, b] = part.astype(jnp.bfloat16)
                y_copy(g, zz).start()

        @pl.loop(0, depth)
        def _(k):
            for b, part in merged(g, k, y):
                banks[g][9][k, b] = part

    def return_column(g):
        @pl.loop(1, depth)
        def _(k):
            to_z = lax.rem(z + k, depth)
            total = banks[g][9][to_z]
            if cols > 1:
                y_copy(g, to_z).wait_recv()
                total = total + banks[g][5][to_z].astype(jnp.float32)
            banks[g][6][to_z] = total.astype(jnp.bfloat16)
            z_copy(g, to_z).start()

        total = banks[g][9][z] + banks[g][1][:own_blocks]
        if cols > 1:
            y_copy(g, z).wait_recv()
            total = total + banks[g][5][z].astype(jnp.float32)
        banks[g][8][...] = total

    def return_end(g):
        @pl.loop(1, depth)
        def _(k):
            from_z = lax.rem(z + depth - k, depth)
            z_arrival(g, from_z).wait_recv()
            banks[g][8][...] += banks[g][7][from_z].astype(jnp.float32)

        whole = banks[g][8][...].reshape(own_rows, dh)
        mix_ref[g % 2, pl.ds(g // 2, own_rows, stride=groups), :] = whole

    def return_drain(g):
        sib_copy(g).wait_send()
        if cols > 1:
            @pl.loop(0, depth)
            def _(k):
                y_copy(g, k).wait_send()

        @pl.loop(1, depth)
        def _(k):
            z_copy(g, lax.rem(z + k, depth)).wait_send()

    barrier = pltpu.get_barrier_semaphore()

    def greet(peer):
        pl.semaphore_signal(
            barrier, inc=1, device_id={"ctx": peer}, device_id_type=pl.DeviceIdType.MESH
        )

    @pl.loop(1, depth)
    def _(k):
        greet(device(lax.rem(z + k, depth), y, core))

    if cols > 1:
        greet(y_peer)
    greet(sib)
    loads = [
        pltpu.make_async_copy(q_hbm, q_ref, in_sem.at[0]),
        pltpu.make_async_copy(do_hbm, do_ref, in_sem.at[1]),
    ]
    for load in loads:
        load.start()
    pl.semaphore_wait(barrier, depth + cols - 1)
    for u in range(units):
        gather_start(u)
    for g in range(groups):
        fill_tables(g, n, me, n_far, own_blocks, sel_ref, picked_ref, tab_ref)
    to_scalars = pltpu.make_async_copy(tab_ref, tab, in_sem.at[2])
    to_scalars.start()
    to_scalars.wait()
    for load in loads:
        load.wait()
    gather_column(0)
    gather_across(0)
    gather_end(0)
    fill = functools.partial(fill_pool, n=n, n_far=n_far, tab=tab, own_kv=own_kv, pool_ref=pool_ref)
    for g in range(groups):
        keys_unit, values_unit = 2 * g, 2 * g + 1
        fill(keys_unit, gathered_ref=banks[keys_unit][0])
        if g > 0:
            return_start(values_unit - 2)
            return_start(keys_unit - 2)
        for i in range(chunks):
            weigh(
                g, per_group, i, chunk_tokens, own_blocks,
                picked_ref, q_ref, do_ref, pool_ref, p_ref, banks[values_unit][1],
            )
            if i == 0:
                gather_column(values_unit)
            if i == min(1, chunks - 1) and g > 0:
                return_across(values_unit - 2)
            if i == min(2, chunks - 1):
                gather_across(values_unit)
                if g > 0:
                    return_across(keys_unit - 2)
        gather_end(values_unit)
        fill(values_unit, gathered_ref=banks[values_unit][0])
        if g + 1 == groups:
            return_start(values_unit)
        for i in range(chunks):
            differentiate(
                g, per_group, i, chunk_tokens,
                q_ref, do_ref, dq_ref, pool_ref, p_ref, banks[keys_unit][1],
            )
            if i == 0:
                if g > 0:
                    return_column(values_unit - 2)
                if g + 1 < groups:
                    gather_column(keys_unit + 2)
            if i == min(1, chunks - 1):
                if g + 1 == groups:
                    return_across(values_unit)
                if g > 0:
                    return_column(keys_unit - 2)
            if i == min(2, chunks - 1) and g + 1 < groups:
                gather_across(keys_unit + 2)
        if g + 1 < groups:
            gather_end(keys_unit + 2)
    last = units - 2
    return_start(last)
    return_column(last + 1)
    return_across(last)
    for u in range(last):
        return_end(u)
    return_column(last)
    return_end(last + 1)
    return_end(last)
    for u in range(units):
        gather_drain(u)
        return_drain(u)
    key_out[...] = mix_ref[0, : own_rows * groups].astype(jnp.bfloat16)
    value_out[...] = mix_ref[1, : own_rows * groups].astype(jnp.bfloat16)


def columns_of(mesh, n):
    spots = [getattr(d, "coords", None) for d in mesh.devices.reshape(-1, n)[0]]
    if None in spots or n % 2:
        return 1
    cols = sum(spot[2] == spots[0][2] for spot in spots) // 2
    return 2 if cols == 2 and n % 4 == 0 else 1


def local(cols, queries, keys, values, grad_out, selected):
    tokens, head_count, dh = queries.shape
    groups = keys.shape[1]
    own_blocks = tokens // BLK
    n = lax.axis_size("ctx")
    depth = n // (2 * cols)
    fetched = min(n - 2, max(selected.shape[2] - own_blocks, 4)) + 1
    chunk_tokens = min(tokens, 32)
    chunk_rows = chunk_tokens * (head_count // groups)
    slots = -(-(own_blocks + fetched) // 16) * 16
    far_rows = -(-fetched // 8) * 8
    pool_rows = (own_blocks + fetched) * BLK
    chosen = selected.transpose(1, 2, 0)
    own_kv = jnp.stack([keys, values], axis=0).transpose(2, 0, 1, 3)
    piece = (own_blocks, BLK, dh)
    units = 2 * groups
    own_kv = own_kv.reshape((units,) + piece)
    vmem = pl.BlockSpec(memory_space=pltpu.VMEM)
    any_spec = pl.BlockSpec(memory_space=pl.ANY)
    bank = [
        pltpu.VMEM((n,) + piece, jnp.bfloat16),
        pltpu.VMEM((pool_rows // BLK, BLK, dh), jnp.float32),
        pltpu.VMEM((n // 2, ID_ROWS + BLK, dh), jnp.bfloat16),
        pltpu.VMEM((n // 2, ID_ROWS + BLK, dh), jnp.bfloat16),
        pltpu.VMEM((depth,) + piece, jnp.bfloat16),
        pltpu.VMEM((depth,) + piece, jnp.bfloat16),
        pltpu.VMEM((depth,) + piece, jnp.bfloat16),
        pltpu.VMEM((depth,) + piece, jnp.bfloat16),
        pltpu.VMEM(piece, jnp.float32),
        pltpu.VMEM((depth,) + piece, jnp.float32),
    ]
    dma = pltpu.SemaphoreType.DMA
    dq, key_grad, value_grad = pl.pallas_call(
        functools.partial(fused_kernel, n, cols, fetched, chunk_tokens, groups),
        out_shape=(
            jax.ShapeDtypeStruct(queries.shape, jnp.bfloat16),
            jax.ShapeDtypeStruct((tokens * groups, dh), jnp.bfloat16),
            jax.ShapeDtypeStruct((tokens * groups, dh), jnp.bfloat16),
        ),
        in_specs=[vmem, any_spec, any_spec, vmem],
        out_specs=(vmem, vmem, vmem),
        scratch_shapes=bank * units + [
            pltpu.VMEM((groups, slots, tokens), jnp.bfloat16),
            pltpu.VMEM((groups, n + far_rows, LANES), jnp.int32),
            pltpu.SMEM((groups, n + far_rows, LANES), jnp.int32),
            pltpu.VMEM(queries.shape, jnp.bfloat16),
            pltpu.VMEM(queries.shape, jnp.bfloat16),
            pltpu.VMEM((2, tokens * groups + 8, dh), jnp.float32),
            dma((3,)),
            pltpu.VMEM((2, pool_rows, dh), jnp.bfloat16),
            pltpu.VMEM((tokens // chunk_tokens, pool_rows, chunk_rows), jnp.float32),
            dma((units, depth)),
            dma((units, depth)),
            dma((units, n)),
            dma((units, n)),
            dma((units, 2)),
            dma((units, depth)),
            dma((units, depth)),
            dma((units, depth)),
            dma((units, depth)),
        ],
        compiler_params=pltpu.CompilerParams(collective_id=0, has_side_effects=True),
    )(chosen, queries, grad_out, own_kv)
    return dq, key_grad.reshape(keys.shape), value_grad.reshape(values.shape)


def solution(mesh):
    spec = P(("rep", "ctx"), None, None)
    cols = columns_of(mesh, mesh.shape["ctx"])
    return jax.shard_map(
        functools.partial(local, cols),
        mesh=mesh,
        in_specs=(spec,) * 5,
        out_specs=(spec,) * 3,
        check_vma=False,
    )
```

```python
import functools
import math

import jax
import jax.numpy as jnp
from jax import lax
from jax.experimental import pallas as pl
from jax.experimental.pallas import tpu as pltpu
from jax.sharding import PartitionSpec as P

BLK = 64
NEG = -1e30
ID_ROWS = 16
LANES = 128
LOG2E = math.log2(math.e)
NT = (((1,), (1,)), ((), ()))
NN = (((1,), (0,)), ((), ()))


def weigh(g, per_group, chunk, chunk_tokens, own_slots, picked_ref, q_ref, do_ref, pool_ref, p_ref, acc_ref):
    tokens, _, dh = q_ref.shape
    keys = pool_ref.shape[1]
    slots = keys // BLK
    log_scale = LOG2E / math.sqrt(dh)
    rows = chunk_tokens * per_group
    shift = per_group.bit_length() - 1
    heads = slice(g * per_group, (g + 1) * per_group)
    t0 = chunk * chunk_tokens
    q = q_ref[t0 : t0 + chunk_tokens, heads, :].reshape(rows, dh)
    do = do_ref[t0 : t0 + chunk_tokens, heads, :].reshape(rows, dh)
    row_tok = t0 + (lax.broadcasted_iota(jnp.int32, (tokens, rows), 1) >> shift)
    tok = lax.broadcasted_iota(jnp.int32, (tokens, rows), 0)
    spread = jnp.where(row_tok == tok, 1.0, 0.0).astype(jnp.bfloat16)
    seen = lax.dot_general(picked_ref[g], spread, NN, preferred_element_type=jnp.float32)
    bias = (seen - 1.0) * (-NEG)
    s = lax.dot_general(pool_ref[0], q, NT, preferred_element_type=jnp.float32)
    pieces = []
    for j in range(slots):
        piece = s[j * BLK : (j + 1) * BLK] + bias[j : j + 1]
        if j < own_slots:
            key_pos = j * BLK + lax.broadcasted_iota(jnp.int32, (BLK, rows), 0)
            piece = jnp.where(key_pos <= row_tok[:BLK], piece, NEG)
        pieces.append(piece)
    s = jnp.concatenate(pieces, axis=0)
    peak = jnp.max(s, axis=0, keepdims=True)
    e = jnp.exp2((s - peak) * log_scale)
    p = e * (1.0 / jnp.sum(e, axis=0, keepdims=True))
    p_ref[chunk] = p
    dv = lax.dot_general(p.astype(jnp.bfloat16), do, NN, preferred_element_type=jnp.float32)
    dv = dv.reshape(slots, BLK, dh)
    acc_ref[...] = dv if chunk == 0 else acc_ref[...] + dv


def differentiate(g, per_group, chunk, chunk_tokens, q_ref, do_ref, dq_ref, pool_ref, p_ref, acc_ref):
    dh = q_ref.shape[2]
    keys = pool_ref.shape[1]
    scaling = 1.0 / math.sqrt(dh)
    rows = chunk_tokens * per_group
    heads = slice(g * per_group, (g + 1) * per_group)
    t0 = chunk * chunk_tokens
    q = q_ref[t0 : t0 + chunk_tokens, heads, :].reshape(rows, dh)
    do = do_ref[t0 : t0 + chunk_tokens, heads, :].reshape(rows, dh)
    p = p_ref[chunk]
    dp = lax.dot_general(pool_ref[1], do, NT, preferred_element_type=jnp.float32)
    inner = jnp.sum(p * dp, axis=0, keepdims=True)
    ds = (p * (dp - inner)).astype(jnp.bfloat16)
    dqt = lax.dot_general(pool_ref[0].T, ds, NN, preferred_element_type=jnp.float32)
    dq = (dqt * scaling).T.astype(jnp.bfloat16)
    dq_ref[t0 : t0 + chunk_tokens, heads, :] = dq.reshape(chunk_tokens, per_group, dh)
    dk = lax.dot_general(ds, q, NN, preferred_element_type=jnp.float32)
    dk = dk.reshape(keys // BLK, BLK, dh)
    acc_ref[...] = dk if chunk == 0 else acc_ref[...] + dk


def fill_tables(g, n, me, n_far, own_blocks, sel_ref, picked_ref, tab_ref):
    sel = sel_ref[g]
    tokens = sel.shape[1]
    shift = own_blocks.bit_length() - 1
    owner = sel >> shift
    block = sel & (own_blocks - 1)
    peers = lax.broadcasted_iota(jnp.int32, (n, tokens), 0)
    code = jnp.zeros((n, tokens), jnp.float32)
    for i in range(sel.shape[0]):
        mark = (block[i : i + 1] + 1).astype(jnp.float32)
        code = jnp.maximum(code, jnp.where(owner[i : i + 1] == peers, mark, 0.0))
    code = jnp.broadcast_to(jnp.max(code, axis=1, keepdims=True), (n, LANES))
    peers = lax.broadcasted_iota(jnp.int32, (n, LANES), 0)
    code = jnp.where(peers == me, 0.0, code)
    live = jnp.where(code > 0.0, 1.0, 0.0)
    before = lax.broadcasted_iota(jnp.int32, (n, n), 1) < lax.broadcasted_iota(jnp.int32, (n, n), 0)
    before = jnp.where(before, 1.0, 0.0).astype(jnp.bfloat16)
    slot = lax.dot_general(before, live.astype(jnp.bfloat16), NN, preferred_element_type=jnp.float32)
    far = jnp.maximum(code - 1.0, 0.0)
    lane = lax.broadcasted_iota(jnp.int32, (n, LANES), 1)
    kept = jnp.minimum(slot, float(n_far - 1))
    entry = jnp.where(lane == 0, kept, jnp.where(lane == 1, live, far))
    tab_ref[g, :n, :] = entry.astype(jnp.int32)
    peer = peers.astype(jnp.float32)
    now = me * own_blocks + (lax.broadcasted_iota(jnp.int32, (1, tokens), 1) >> BLK.bit_length() - 1)
    slots = picked_ref.shape[1]
    row = lax.broadcasted_iota(jnp.int32, (slots, tokens), 0)
    far_rows = tab_ref.shape[1] - n
    far_row = lax.broadcasted_iota(jnp.int32, (far_rows, LANES), 0)
    far_lane = lax.broadcasted_iota(jnp.int32, (far_rows, LANES), 1)
    far_entry = jnp.zeros((far_rows, LANES), jnp.float32)
    picked = jnp.zeros((slots, tokens), jnp.float32)
    for i in range(own_blocks + n_far):
        if i < own_blocks:
            ids = jnp.full((1, tokens), me * own_blocks + i, jnp.int32)
        else:
            hit = (live > 0.0) & (slot == float(i - own_blocks))
            who = jnp.max(jnp.where(hit, peer, -1.0), axis=0, keepdims=True)
            which = jnp.max(jnp.where(hit, far, 0.0), axis=0, keepdims=True)
            ids = jnp.max(who * own_blocks + which, axis=1, keepdims=True).astype(jnp.int32)
            ids = jnp.broadcast_to(ids, (1, tokens))
            here = jnp.where(far_lane == 0, jnp.maximum(who, 0.0), which)
            far_entry = jnp.where(far_row == i - own_blocks, here, far_entry)
        seen = jnp.max(jnp.where(sel == ids, 1.0, 0.0), axis=0, keepdims=True)
        seen = jnp.where(ids <= now, seen, 0.0)
        picked = jnp.where(row == i, seen, picked)
    tab_ref[g, n:, :] = far_entry.astype(jnp.int32)
    picked_ref[g] = picked.astype(jnp.bfloat16)


def fill_pool(unit, n, n_far, tab, own_kv, gathered_ref, pool_ref):
    group, kv = divmod(unit, 2)
    own_blocks = own_kv.shape[1]
    own_rows = own_blocks * BLK
    pool_ref[kv, :own_rows, :] = own_kv[unit].reshape(own_rows, own_kv.shape[3])
    for s in range(n_far):
        owner = jnp.clip(tab[group, n + s, 0], 0, n - 1)
        block = jnp.clip(tab[group, n + s, 1], 0, own_blocks - 1)
        lo = own_rows + s * BLK
        pool_ref[kv, lo : lo + BLK, :] = gathered_ref[owner, block]


def fused_kernel(
    n, cols, n_far, chunk_tokens, groups,
    sel_ref, q_hbm, do_hbm, own_kv, dq_ref, key_out, value_out, *scratch,
):
    per_bank = 10
    units = 2 * groups
    banks = [scratch[g * per_bank : (g + 1) * per_bank] for g in range(units)]
    (
        picked_ref, tab_ref, tab, q_ref, do_ref, mix_ref, in_sem, pool_ref, p_ref, col_send, y_send, sib_send, recv_sem,
        rs_sem, ry_send, ry_recv, rz_send, rz_recv,
    ) = scratch[units * per_bank :]
    depth = n // (2 * cols)
    chips = n // 2
    me = lax.axis_index("ctx")
    core = lax.rem(me, 2)
    chip = me // 2
    y = lax.rem(chip, cols)
    z = chip // cols
    sib = 2 * chip + 1 - core
    other_y = cols - 1 - y
    y_peer = 2 * (z * cols + other_y) + core
    own_blocks = own_kv.shape[1]
    own_rows = own_blocks * BLK
    dh = own_kv.shape[3]
    per_group = q_ref.shape[1] // groups
    chunks = q_ref.shape[0] // chunk_tokens
    scaling = 1.0 / math.sqrt(dh)

    def device(zz, yy, cc):
        return 2 * (zz * cols + yy) + cc

    def remote(src, dst, send, recv, peer):
        return pltpu.make_async_remote_copy(
            src_ref=src,
            dst_ref=dst,
            send_sem=send,
            recv_sem=recv,
            device_id={"ctx": peer},
            device_id_type=pl.DeviceIdType.MESH,
        )

    def col_copy(g, k):
        peer = device(lax.rem(z + k, depth), y, core)
        return remote(
            own_kv.at[g], banks[g][0].at[me], col_send.at[g, k], recv_sem.at[g, me], peer
        )

    def own_copy(g, sem, peer):
        return remote(own_kv.at[g], banks[g][0].at[me], sem, recv_sem.at[g, me], peer)

    def pass_on(g, src, sem, peer):
        slot = banks[g][0].at[src]
        return remote(slot, slot, sem, recv_sem.at[g, src], peer)

    def await_piece(g, src):
        pass_on(g, src, sib_send.at[g, src], sib).wait_recv()

    def gather_start(g):
        if cols > 1:
            own_copy(g, y_send.at[g, z], y_peer).start()

        @pl.loop(1, depth)
        def _(k):
            col_copy(g, k).start()

        own_copy(g, sib_send.at[g, me], sib).start()

    def gather_column(g):
        @pl.loop(1, depth)
        def _(k):
            from_z = lax.rem(z + depth - k, depth)
            src = device(from_z, y, core)
            await_piece(g, src)
            if cols > 1:
                pass_on(g, src, y_send.at[g, from_z], y_peer).start()
            pass_on(g, src, sib_send.at[g, src], sib).start()

    def gather_across(g):
        if cols > 1:
            @pl.loop(0, depth)
            def _(k):
                src = device(lax.rem(z + depth - k, depth), other_y, core)
                await_piece(g, src)
                pass_on(g, src, sib_send.at[g, src], sib).start()

    def gather_end(g):
        @pl.loop(0, chips)
        def _(q):
            await_piece(g, 2 * q + 1 - core)

    def gather_drain(g):
        @pl.loop(1, depth)
        def _(k):
            col_copy(g, k).wait_send()

        if cols > 1:
            @pl.loop(0, depth)
            def _(k):
                pass_on(g, device(k, y, core), y_send.at[g, k], y_peer).wait_send()

        @pl.loop(0, chips)
        def _(q):
            src = 2 * q + core
            pass_on(g, src, sib_send.at[g, src], sib).wait_send()

    def sib_copy(g):
        return remote(banks[g][2], banks[g][3], rs_sem.at[g, 0], rs_sem.at[g, 1], sib)

    def y_copy(g, k):
        return remote(
            banks[g][4].at[k], banks[g][5].at[k], ry_send.at[g, k], ry_recv.at[g, k], y_peer
        )

    def z_copy(g, to_z):
        peer = device(to_z, y, core)
        return remote(
            banks[g][6].at[to_z], banks[g][7].at[z], rz_send.at[g, to_z], rz_recv.at[g, z], peer
        )

    def z_arrival(g, from_z):
        peer = device(from_z, y, core)
        return remote(
            banks[g][6].at[from_z], banks[g][7].at[from_z],
            rz_send.at[g, from_z], rz_recv.at[g, from_z], peer,
        )

    def far_part(g, dest):
        return banks[g][1][own_blocks + jnp.clip(tab[g // 2, dest, 0], 0, n_far - 1)]

    def return_start(g):
        acc_ref, box = banks[g][1], banks[g][2]
        if g % 2 == 0:
            acc_ref[...] = acc_ref[...] * scaling

        @pl.loop(0, chips)
        def _(q):
            dest = 2 * q + 1 - core
            keep = tab[g // 2, dest, 1].astype(jnp.float32)
            block = tab[g // 2, dest, 2].astype(jnp.float32)
            box[q, :ID_ROWS, :] = jnp.full((ID_ROWS, dh), block, jnp.float32).astype(jnp.bfloat16)
            box[q, ID_ROWS:, :] = (far_part(g, dest) * keep).astype(jnp.bfloat16)

        sib_copy(g).start()

    def merged(g, zz, yy):
        q = zz * cols + yy
        dest = 2 * q + core
        box = banks[g][3]
        which = box[q, :ID_ROWS, :].astype(jnp.float32)[:1]
        keep = tab[g // 2, dest, 1].astype(jnp.float32)
        block = jnp.full((1, dh), tab[g // 2, dest, 2].astype(jnp.float32), jnp.float32)
        theirs = box[q, ID_ROWS:, :].astype(jnp.float32)
        mine = far_part(g, dest) * keep
        for b in range(own_blocks):
            yield b, (
                jnp.where(block == float(b), mine, 0.0) + jnp.where(which == float(b), theirs, 0.0)
            )

    def return_across(g):
        sib_copy(g).wait_recv()
        if cols > 1:
            @pl.loop(0, depth)
            def _(k):
                zz = lax.rem(z + 1 + k, depth)
                for b, part in merged(g, zz, other_y):
                    banks[g][4][zz, b] = part.astype(jnp.bfloat16)
                y_copy(g, zz).start()

        @pl.loop(0, depth)
        def _(k):
            for b, part in merged(g, k, y):
                banks[g][9][k, b] = part

    def return_column(g):
        @pl.loop(1, depth)
        def _(k):
            to_z = lax.rem(z + k, depth)
            total = banks[g][9][to_z]
            if cols > 1:
                y_copy(g, to_z).wait_recv()
                total = total + banks[g][5][to_z].astype(jnp.float32)
            banks[g][6][to_z] = total.astype(jnp.bfloat16)
            z_copy(g, to_z).start()

        total = banks[g][9][z] + banks[g][1][:own_blocks]
        if cols > 1:
            y_copy(g, z).wait_recv()
            total = total + banks[g][5][z].astype(jnp.float32)
        banks[g][8][...] = total

    def return_end(g):
        @pl.loop(1, depth)
        def _(k):
            from_z = lax.rem(z + depth - k, depth)
            z_arrival(g, from_z).wait_recv()
            banks[g][8][...] += banks[g][7][from_z].astype(jnp.float32)

        whole = banks[g][8][...].reshape(own_rows, dh)
        mix_ref[g % 2, pl.ds(g // 2, own_rows, stride=groups), :] = whole

    def return_drain(g):
        sib_copy(g).wait_send()
        if cols > 1:
            @pl.loop(0, depth)
            def _(k):
                y_copy(g, k).wait_send()

        @pl.loop(1, depth)
        def _(k):
            z_copy(g, lax.rem(z + k, depth)).wait_send()

    barrier = pltpu.get_barrier_semaphore()

    def greet(peer):
        pl.semaphore_signal(
            barrier, inc=1, device_id={"ctx": peer}, device_id_type=pl.DeviceIdType.MESH
        )

    @pl.loop(1, depth)
    def _(k):
        greet(device(lax.rem(z + k, depth), y, core))

    if cols > 1:
        greet(y_peer)
    greet(sib)
    loads = [
        pltpu.make_async_copy(q_hbm, q_ref, in_sem.at[0]),
        pltpu.make_async_copy(do_hbm, do_ref, in_sem.at[1]),
    ]
    for load in loads:
        load.start()
    pl.semaphore_wait(barrier, depth + cols - 1)
    for u in range(units):
        gather_start(u)
    for g in range(groups):
        fill_tables(g, n, me, n_far, own_blocks, sel_ref, picked_ref, tab_ref)
    to_scalars = pltpu.make_async_copy(tab_ref, tab, in_sem.at[2])
    to_scalars.start()
    to_scalars.wait()
    for load in loads:
        load.wait()
    gather_column(0)
    gather_column(1)
    gather_across(0)
    gather_across(1)
    gather_end(0)
    fill = functools.partial(fill_pool, n=n, n_far=n_far, tab=tab, own_kv=own_kv, pool_ref=pool_ref)
    for g in range(groups):
        keys_unit, values_unit = 2 * g, 2 * g + 1
        fill(keys_unit, gathered_ref=banks[keys_unit][0])
        for i in range(chunks):
            weigh(
                g, per_group, i, chunk_tokens, own_blocks,
                picked_ref, q_ref, do_ref, pool_ref, p_ref, banks[values_unit][1],
            )
            if g + 1 < groups:
                if i == 0:
                    gather_column(keys_unit + 2)
                if i == min(1, chunks - 1):
                    gather_column(values_unit + 2)
                if i == min(2, chunks - 1):
                    gather_across(keys_unit + 2)
                if i == chunks - 1:
                    gather_across(values_unit + 2)
            if g > 0:
                if i == 0:
                    return_across(keys_unit - 2)
                    return_column(values_unit - 2)
                if i == min(2, chunks - 1):
                    return_column(keys_unit - 2)
        gather_end(values_unit)
        fill(values_unit, gathered_ref=banks[values_unit][0])
        return_start(values_unit)
        for i in range(chunks):
            differentiate(
                g, per_group, i, chunk_tokens,
                q_ref, do_ref, dq_ref, pool_ref, p_ref, banks[keys_unit][1],
            )
            if i == min(1, chunks - 1):
                return_across(values_unit)
            if i == chunks - 1 and g + 1 == groups:
                return_start(keys_unit)
                return_column(values_unit)
        if g + 1 < groups:
            return_start(keys_unit)
            gather_end(keys_unit + 2)
    last = units - 2
    return_across(last)
    for u in range(last):
        return_end(u)
    return_column(last)
    return_end(last + 1)
    return_end(last)
    for u in range(units):
        gather_drain(u)
        return_drain(u)
    key_out[...] = mix_ref[0, : own_rows * groups].astype(jnp.bfloat16)
    value_out[...] = mix_ref[1, : own_rows * groups].astype(jnp.bfloat16)


def columns_of(mesh, n):
    spots = [getattr(d, "coords", None) for d in mesh.devices.reshape(-1, n)[0]]
    if None in spots or n % 2:
        return 1
    cols = sum(spot[2] == spots[0][2] for spot in spots) // 2
    return 2 if cols == 2 and n % 4 == 0 else 1


def local(cols, queries, keys, values, grad_out, selected):
    tokens, head_count, dh = queries.shape
    groups = keys.shape[1]
    own_blocks = tokens // BLK
    n = lax.axis_size("ctx")
    depth = n // (2 * cols)
    fetched = min(n - 2, max(selected.shape[2] - own_blocks, 4)) + 1
    chunk_tokens = min(tokens, 32)
    chunk_rows = chunk_tokens * (head_count // groups)
    slots = -(-(own_blocks + fetched) // 16) * 16
    far_rows = -(-fetched // 8) * 8
    pool_rows = (own_blocks + fetched) * BLK
    chosen = selected.transpose(1, 2, 0)
    own_kv = jnp.stack([keys, values], axis=0).transpose(2, 0, 1, 3)
    piece = (own_blocks, BLK, dh)
    units = 2 * groups
    own_kv = own_kv.reshape((units,) + piece)
    vmem = pl.BlockSpec(memory_space=pltpu.VMEM)
    any_spec = pl.BlockSpec(memory_space=pl.ANY)
    bank = [
        pltpu.VMEM((n,) + piece, jnp.bfloat16),
        pltpu.VMEM((pool_rows // BLK, BLK, dh), jnp.float32),
        pltpu.VMEM((n // 2, ID_ROWS + BLK, dh), jnp.bfloat16),
        pltpu.VMEM((n // 2, ID_ROWS + BLK, dh), jnp.bfloat16),
        pltpu.VMEM((depth,) + piece, jnp.bfloat16),
        pltpu.VMEM((depth,) + piece, jnp.bfloat16),
        pltpu.VMEM((depth,) + piece, jnp.bfloat16),
        pltpu.VMEM((depth,) + piece, jnp.bfloat16),
        pltpu.VMEM(piece, jnp.float32),
        pltpu.VMEM((depth,) + piece, jnp.float32),
    ]
    dma = pltpu.SemaphoreType.DMA
    dq, key_grad, value_grad = pl.pallas_call(
        functools.partial(fused_kernel, n, cols, fetched, chunk_tokens, groups),
        out_shape=(
            jax.ShapeDtypeStruct(queries.shape, jnp.bfloat16),
            jax.ShapeDtypeStruct((tokens * groups, dh), jnp.bfloat16),
            jax.ShapeDtypeStruct((tokens * groups, dh), jnp.bfloat16),
        ),
        in_specs=[vmem, any_spec, any_spec, vmem],
        out_specs=(vmem, vmem, vmem),
        scratch_shapes=bank * units + [
            pltpu.VMEM((groups, slots, tokens), jnp.bfloat16),
            pltpu.VMEM((groups, n + far_rows, LANES), jnp.int32),
            pltpu.SMEM((groups, n + far_rows, LANES), jnp.int32),
            pltpu.VMEM(queries.shape, jnp.bfloat16),
            pltpu.VMEM(queries.shape, jnp.bfloat16),
            pltpu.VMEM((2, tokens * groups + 8, dh), jnp.float32),
            dma((3,)),
            pltpu.VMEM((2, pool_rows, dh), jnp.bfloat16),
            pltpu.VMEM((tokens // chunk_tokens, pool_rows, chunk_rows), jnp.float32),
            dma((units, depth)),
            dma((units, depth)),
            dma((units, n)),
            dma((units, n)),
            dma((units, 2)),
            dma((units, depth)),
            dma((units, depth)),
            dma((units, depth)),
            dma((units, depth)),
        ],
        compiler_params=pltpu.CompilerParams(collective_id=0, has_side_effects=True),
    )(chosen, queries, grad_out, own_kv)
    return dq, key_grad.reshape(keys.shape), value_grad.reshape(values.shape)


def solution(mesh):
    spec = P(("rep", "ctx"), None, None)
    cols = columns_of(mesh, mesh.shape["ctx"])
    return jax.shard_map(
        functools.partial(local, cols),
        mesh=mesh,
        in_specs=(spec,) * 5,
        out_specs=(spec,) * 3,
        check_vma=False,
    )
```
